32 devices in a mesh: section: 2 (over core), dp: 8 (over z, x), rep: 2 (over y).
Axes of the slice: x: 2, y: 2, z: 4, core: 2. Of those that a mesh axis runs over, the one named last changes fastest.
Arguments:
- patches: bfloat16 [64, 196, 768], P(('dp', 'rep'), None, 'section'), may hold values from -6 to 6
- captions: bfloat16 [64, 128, 768], P(('dp', 'rep'), None, 'section'), may hold values from -6 to 6
- tissue_keep: int32 [64, 196], P(('dp', 'rep')), may hold values from 0 to 1, as said below
- caption_mask: int32 [64, 128], P(('dp', 'rep')), may hold values from 0 to 1, as said below
- mixing: bfloat16 [2, 768, 2304], P('section', 'dp'), may hold values from -0.21875 to 0.21875
- merging: bfloat16 [2, 768, 768], P('section', 'dp'), may hold values from -0.875 to 0.875
- crossing: bfloat16 [2, 768, 1536], P('section', 'dp'), may hold values from -0.21875 to 0.21875
- widening: bfloat16 [2, 768, 3072], P('section', 'dp'), may hold values from -0.21875 to 0.21875
- narrowing: bfloat16 [2, 3072, 768], P('section', 'dp'), may hold values from -0.109375 to 0.109375
- scales: bfloat16 [2, 3, 768], P('section', None, 'dp'), may hold values from 0.5 to 1.5
- cotangent: bfloat16 [64, 128, 768], P(('dp', 'rep'), None, 'section'), may hold values from -6 to 6
Outputs:
- decoded: bfloat16 [64, 128, 768], P(('dp', 'rep'), None, 'section')
- caption_grad: bfloat16 [64, 128, 768], P(('dp', 'rep'), None, 'section')
- patch_grad: bfloat16 [64, 196, 768], P(('dp', 'rep'), None, 'section')
- mixing_grad: float32 [2, 768, 2304], P('section', 'dp')
- merging_grad: float32 [2, 768, 768], P('section', 'dp')
- crossing_grad: float32 [2, 768, 1536], P('section', 'dp')
- widening_grad: float32 [2, 768, 3072], P('section', 'dp')
- narrowing_grad: float32 [2, 3072, 768], P('section', 'dp')
- scales_grad: float32 [2, 3, 768], P('section', None, 'dp')
The draws below stay inside these ranges and needn't reach their ends.
Inputs may be any that keep to these rules, and one draw needn't show every extreme that they name: `tissue_keep`: every image keeps between 24 and 196 patches, in any places; some image keeps exactly 24, some all. `caption_mask`: each caption's mask is 1 on a prefix of 8 to 128 positions and 0 after it; both ends are reached.
All inputs are finite; a program needn't handle non-finite values.
Results may differ from the reference program's by a relative error of at most 0.019.
Values may be sent and summed in bfloat16 or wider, within the bound.
A program may use at most 320 MiB of HBM per device.

```python
import jax
import jax.numpy as jnp
from jax import lax

D = 768
FF = 3072
HEADS = 12
PATCHES = 196
TEXT_LEN = 128
IMG_MB = 2
MICRO = 2
IMAGES = 64


def draw_tissue_keep(key, part):
    count_key, other_key, order_key = jax.random.split(jax.random.fold_in(key, 11), 3)
    least = PATCHES // 8
    spread = PATCHES - least
    first_pick = jax.random.randint(count_key, (IMAGES,), 0, spread + 1)
    second_pick = jax.random.randint(other_key, (IMAGES,), 0, spread + 1)
    counts = least + first_pick * second_pick // spread
    counts = counts.at[0].set(least).at[1].set(PATCHES)
    ranks = jax.vmap(lambda sub: jax.random.permutation(sub, PATCHES))(jax.random.split(order_key, IMAGES))
    return (ranks < counts[:, None]).astype(jnp.int32)


def draw_caption_mask(key, part):
    least = max(1, TEXT_LEN // 16)
    lengths = jax.random.randint(jax.random.fold_in(key, 23), (IMAGES,), least, TEXT_LEN + 1)
    lengths = lengths.at[0].set(least).at[1].set(TEXT_LEN)
    positions = jnp.arange(TEXT_LEN, dtype=jnp.int32)
    return (positions[None, :] < lengths[:, None]).astype(jnp.int32)


def levels(rng, extent, cuts, low, largest):
    level = 1.0
    for axis_at, shards_of in cuts:
        steps = jax.random.uniform(jax.random.fold_in(jax.random.fold_in(rng, 6), axis_at), (shards_of,), jnp.float32, low / len(cuts), largest / len(cuts))
        level = level * jnp.repeat(jnp.exp(steps), extent[axis_at] // shards_of).reshape((-1,) + (1,) * (len(extent) - 1 - axis_at))
    return level


def noise(own_key, shape, scale, reach, cuts=(), kind=jnp.bfloat16):
    result = jax.random.normal(own_key, shape, jnp.float32) * scale
    if len(cuts) > 0:
        result = levels(own_key, shape, cuts, -0.22, 0.18) * result
    return jnp.clip(result, min=-reach, max=reach).astype(kind)


def setup_inputs(seed: int = 0) -> dict:
    streams_of = jax.random.split(jax.random.key(seed), 12)
    patches = noise(streams_of[0], (IMAGES, PATCHES, D), 1.0, 6.0, ((0, 16), (2, 2)))
    captions = noise(streams_of[1], (IMAGES, TEXT_LEN, D), 1.0, 6.0, ((0, 16), (2, 2)))
    tissue_keep = draw_tissue_keep(jax.random.fold_in(streams_of[11], 71), 0)
    caption_mask = draw_caption_mask(jax.random.fold_in(streams_of[11], 71), 0)
    mixing = noise(streams_of[4], (2, D, 3 * D), D ** -0.5, 0.21875, ((0, 2), (1, 8)))
    merging = noise(streams_of[5], (2, D, D), (D // 16) ** -0.5, 0.875, ((0, 2), (1, 8)))
    crossing = noise(streams_of[6], (2, D, 2 * D), D ** -0.5, 0.21875, ((0, 2), (1, 8)))
    widening = noise(streams_of[7], (2, D, FF), D ** -0.5, 0.21875, ((0, 2), (1, 8)))
    narrowing = noise(streams_of[8], (2, FF, D), FF ** -0.5, 0.109375, ((0, 2), (1, 8)))
    scales = jnp.clip(1.0 + 0.1 * jax.random.normal(streams_of[9], (2, 3, D), jnp.float32), 0.5, 1.5).astype(jnp.bfloat16)
    cotangent = noise(streams_of[10], (IMAGES, TEXT_LEN, D), 1.0, 6.0, ((0, 16), (2, 2)))
    return {"patches": patches, "captions": captions, "tissue_keep": tissue_keep, "caption_mask": caption_mask, "mixing": mixing, "merging": merging, "crossing": crossing, "widening": widening, "narrowing": narrowing, "scales": scales, "cotangent": cotangent}


@jax.custom_vjp
def low(v):
    return lax.optimization_barrier(v.astype(jnp.bfloat16)).astype(jnp.float32)

@jax.custom_vjp
def low_back(v):
    return v

def low_keep(v):
    return (low(v), None)

def low_pass(kept, grad):
    return (grad,)

def back_keep(v):
    return (v, None)

def back_low(kept, grad):
    return (low(grad),)
low.defvjp(low_keep, low_pass)
low_back.defvjp(back_keep, back_low)

def layer_norm(values, gain):
    centered = values - lax.optimization_barrier(jnp.mean(values, axis=-1, keepdims=True))
    return centered * lax.rsqrt(lax.optimization_barrier(jnp.mean(centered * centered, axis=-1, keepdims=True)) + 1e-05) * gain

def linear(acts, weight):
    return jnp.einsum('bsd,de->bse', acts, weight, precision=lax.Precision.HIGHEST)

def split_heads(values):
    return values.reshape(values.shape[0], values.shape[1], HEADS, values.shape[2] // HEADS)

def attention(queries, keys, values, mask):
    scale = queries.shape[-1] ** (-0.5)
    scores = low_back(jnp.einsum('bqhe,bkhe->bhqk', queries, keys, precision=lax.Precision.HIGHEST) * scale)
    scores = jnp.where(mask[:, None], scores, -1000000000.0)
    softmaxed = jax.nn.softmax(scores, axis=-1)
    mixed = jnp.einsum('bhqk,bkhe->bqhe', low(softmaxed), values, precision=lax.Precision.HIGHEST)
    mixed = low(low_back(mixed))
    return mixed.reshape(mixed.shape[0], mixed.shape[1], -1)

def self_branch(states, gain, w_in, w_out, mask):
    width = states.shape[2]
    first = low(layer_norm(states, gain))
    united = low(low_back(linear(first, w_in)))
    mixed = attention(split_heads(united[..., :width]), split_heads(united[..., width:2 * width]), split_heads(united[..., 2 * width:]), mask)
    return states + low_back(linear(mixed, w_out))

def feed_branch(states, gain, w_up, w_down):
    second = low(layer_norm(states, gain))
    widened = low_back(linear(second, w_up))
    active = low(jax.nn.gelu(widened, approximate=False))
    return states + low_back(linear(active, w_down))

def encode(states, keep, weights):
    w_in, w_out, w_pair, w_up, w_down, gains = weights
    batch, count, width = states.shape
    mask = jnp.broadcast_to(keep[:, None, :] > 0, (batch, count, count))
    hidden = self_branch(states, gains[0], w_in, w_out, mask)
    after = feed_branch(hidden, gains[1], w_up, w_down)
    final = low(layer_norm(after, gains[2]))
    return low(low_back(linear(final, w_pair)))

def decode(text, text_keep, memory, keep, weights):
    w_in, w_out, w_pair, w_up, w_down, gains = weights
    batch, length, width = text.shape
    query_pos = lax.broadcasted_iota(jnp.int32, (length, length), 0)
    key_pos = lax.broadcasted_iota(jnp.int32, (length, length), 1)
    self_mask = (key_pos <= query_pos)[None] & (text_keep[:, None, :] > 0)
    cross_mask = jnp.broadcast_to(keep[:, None, :] > 0, (batch, length, keep.shape[1]))
    hidden = self_branch(text, gains[0], w_in, w_out, self_mask)
    second = low(layer_norm(hidden, gains[1]))
    cross_q = low(low_back(linear(second, w_pair[:, :width])))
    mixed = attention(split_heads(cross_q), split_heads(memory[..., :width]), split_heads(memory[..., width:]), cross_mask)
    crossed = hidden + low_back(linear(mixed, w_pair[:, width:]))
    return feed_branch(crossed, gains[2], w_up, w_down)

def reference(patches, captions, tissue_keep, caption_mask, mixing, merging, crossing, widening, narrowing, scales, cotangent):
    params = tuple((w.astype(jnp.float32) for w in (mixing, merging, crossing, widening, narrowing, scales)))
    group = IMG_MB * MICRO
    groups = IMAGES // group

    def forward(params, patch_vals, text_vals):

        def one_group(items):
            patch_group, text_group, keep_group, mask_group = items
            enc_weights = tuple((w[0] for w in params))
            dec_weights = tuple((w[1] for w in params))
            memory = encode(patch_group, keep_group, enc_weights)
            return decode(text_group, mask_group, memory, keep_group, dec_weights)
        stacked = lax.map(jax.checkpoint(one_group), (patch_vals.reshape(groups, group, PATCHES, D), text_vals.reshape(groups, group, TEXT_LEN, D), tissue_keep.reshape(groups, group, PATCHES), caption_mask.reshape(groups, group, TEXT_LEN)))
        return stacked.reshape(IMAGES, TEXT_LEN, D)
    output, pullback = jax.vjp(forward, params, patches.astype(jnp.float32), captions.astype(jnp.float32))
    grad_params, grad_patches, grad_text = pullback(cotangent.astype(jnp.float32))
    return (output.astype(jnp.bfloat16), grad_text.astype(jnp.bfloat16), grad_patches.astype(jnp.bfloat16), grad_params[0], grad_params[1], grad_params[2], grad_params[3], grad_params[4], grad_params[5])
```

```python
import jax
import jax.numpy as jnp
from jax import lax
from jax.sharding import PartitionSpec as P

HEADS = 12


def partner(value, axis, distance):
    mask = 2**distance
    pairs = [(source, source ^ mask) for source in range(lax.axis_size(axis))]
    return lax.ppermute(value, axis, pairs)


def to_low(values):
    return values.astype(jnp.bfloat16)


def layer_norm(values, gain):
    centered = values - jnp.mean(values, axis=-1, keepdims=True)
    return (
        centered * lax.rsqrt(jnp.mean(centered * centered, axis=-1, keepdims=True) + 1e-05) * gain
    )


def gelu_exact(values):
    return jax.nn.gelu(values, approximate=False)


def project(acts, weight):
    return jnp.einsum("bsd,de->bse", acts, weight, preferred_element_type=jnp.float32)


def back_project(grads, weight):
    return jnp.einsum("bse,de->bsd", grads, weight, preferred_element_type=jnp.float32)


def weight_grad(acts, grads):
    return jnp.einsum("bsd,bse->de", acts, grads, preferred_element_type=jnp.float32)


def split_heads(values):
    return values.reshape(values.shape[0], values.shape[1], HEADS, values.shape[2] // HEADS)


def attend_forward(queries, keys, values, mask):
    scale = queries.shape[-1] ** (-0.5)
    scores = (
        jnp.einsum("bqhe,bkhe->bhqk", queries, keys, preferred_element_type=jnp.float32) * scale
    )
    scores = jnp.where(mask[:, None], scores, -1000000000.0)
    peak = jnp.max(scores, axis=-1, keepdims=True)
    expo = jnp.exp(scores - peak)
    softmaxed = expo / jnp.sum(expo, axis=-1, keepdims=True)
    mixed = jnp.einsum(
        "bhqk,bkhe->bqhe", to_low(softmaxed), values, preferred_element_type=jnp.float32
    )
    return (to_low(mixed), softmaxed)


def attend_backward(grad_mixed, softmaxed, queries, keys, values, mask):
    scale = queries.shape[-1] ** (-0.5)
    grad_soft = jnp.einsum(
        "bqhe,bkhe->bhqk", grad_mixed, values, preferred_element_type=jnp.float32
    )
    grad_value = jnp.einsum(
        "bhqk,bqhe->bkhe", to_low(softmaxed), grad_mixed, preferred_element_type=jnp.float32
    )
    grad_scores = softmaxed * (grad_soft - jnp.sum(softmaxed * grad_soft, axis=-1, keepdims=True))
    grad_scores = to_low(jnp.where(mask[:, None], grad_scores, 0.0))
    grad_query = (
        jnp.einsum("bhqk,bkhe->bqhe", grad_scores, keys, preferred_element_type=jnp.float32) * scale
    )
    grad_key = (
        jnp.einsum("bhqk,bqhe->bkhe", grad_scores, queries, preferred_element_type=jnp.float32)
        * scale
    )
    return (grad_query, grad_key, grad_value)


def attention_forward(states, gain, w_in, w_out, mask):
    width = states.shape[2]
    first = to_low(layer_norm(states, gain))
    united = to_low(project(first, w_in))
    queries = split_heads(united[..., :width])
    keys = split_heads(united[..., width : 2 * width])
    values = split_heads(united[..., 2 * width :])
    mixed, softmaxed = attend_forward(queries, keys, values, mask)
    joined = mixed.reshape(states.shape)
    hidden = states + project(joined, w_out)
    return (first, queries, keys, values, softmaxed, joined, hidden)


def feedforward_forward(states, gain, w_up, w_down):
    second = to_low(layer_norm(states, gain))
    widened = project(second, w_up)
    active = to_low(gelu_exact(widened))
    after = states + project(active, w_down)
    return (second, widened, active, after)


def attention_back(
    grad_after, states, gain, first, queries, keys, values, softmaxed, joined, mask, w_in, w_out
):
    branch = to_low(grad_after)
    g_out = weight_grad(joined, branch)
    grad_joined = to_low(back_project(branch, w_out))
    grad_query, grad_key, grad_value = attend_backward(
        split_heads(grad_joined), softmaxed, queries, keys, values, mask
    )
    shape = states.shape
    grad_united = to_low(
        jnp.concatenate(
            [grad_query.reshape(shape), grad_key.reshape(shape), grad_value.reshape(shape)], axis=-1
        )
    )
    g_in = weight_grad(first, grad_united)
    _, pull = jax.vjp(layer_norm, states, gain)
    grad_norm, g_gain = pull(back_project(grad_united, w_in))
    return (grad_after + grad_norm, g_in, g_out, g_gain)


def feedforward_back(grad_after, states, gain, second, widened, active, w_up, w_down):
    branch = to_low(grad_after)
    g_down = weight_grad(active, branch)
    _, pull = jax.vjp(gelu_exact, widened)
    grad_wide = to_low(pull(back_project(branch, w_down))[0])
    g_up = weight_grad(second, grad_wide)
    _, pull = jax.vjp(layer_norm, states, gain)
    grad_norm, g_gain = pull(back_project(grad_wide, w_up))
    return (grad_after + grad_norm, g_up, g_down, g_gain)


def encoder_pass(states, keep, weights):
    w_in, w_out, w_pair, w_up, w_down, gains = weights
    gains = gains.astype(jnp.float32)
    batch, count, width = states.shape
    mask = jnp.broadcast_to(keep[:, None, :] > 0, (batch, count, count))
    first, queries, keys, values, softmaxed, joined, hidden = attention_forward(
        states, gains[0], w_in, w_out, mask
    )
    second, widened, active, after = feedforward_forward(hidden, gains[1], w_up, w_down)
    final = to_low(layer_norm(after, gains[2]))
    memory = to_low(project(final, w_pair))
    saved = (
        mask,
        first,
        queries,
        keys,
        values,
        softmaxed,
        joined,
        hidden,
        second,
        widened,
        active,
        after,
        final,
    )
    return (memory, saved)


def encoder_backward(states, saved, weights, grad_memory):
    w_in, w_out, w_pair, w_up, w_down, gains = weights
    gains = gains.astype(jnp.float32)
    (
        mask,
        first,
        queries,
        keys,
        values,
        softmaxed,
        joined,
        hidden,
        second,
        widened,
        active,
        after,
        final,
    ) = saved
    g_pair = weight_grad(final, grad_memory)
    _, pull = jax.vjp(layer_norm, after, gains[2])
    grad_after, g_final = pull(back_project(grad_memory, w_pair))
    grad_hidden, g_up, g_down, g_second = feedforward_back(
        grad_after, hidden, gains[1], second, widened, active, w_up, w_down
    )
    grad_states, g_in, g_out, g_first = attention_back(
        grad_hidden,
        states,
        gains[0],
        first,
        queries,
        keys,
        values,
        softmaxed,
        joined,
        mask,
        w_in,
        w_out,
    )
    return (
        grad_states,
        (g_in, g_out, g_pair, g_up, g_down, jnp.stack([g_first, g_second, g_final])),
    )


def decoder_step(text, text_keep, memory, keep, weights, cotan):
    w_in, w_out, w_pair, w_up, w_down, gains = weights
    gains = gains.astype(jnp.float32)
    batch, length, width = text.shape
    query_pos = lax.broadcasted_iota(jnp.int32, (length, length), 0)
    key_pos = lax.broadcasted_iota(jnp.int32, (length, length), 1)
    self_mask = (key_pos <= query_pos)[None] & (text_keep[:, None, :] > 0)
    cross_mask = jnp.broadcast_to(keep[:, None, :] > 0, (batch, length, keep.shape[1]))
    first, queries, keys, values, softmaxed, joined, hidden = attention_forward(
        text, gains[0], w_in, w_out, self_mask
    )
    second = to_low(layer_norm(hidden, gains[1]))
    cross_query = to_low(project(second, w_pair[:, :width]))
    memory_keys = split_heads(memory[..., :width])
    memory_vals = split_heads(memory[..., width:])
    cross_mixed, cross_soft = attend_forward(
        split_heads(cross_query), memory_keys, memory_vals, cross_mask
    )
    cross_joined = cross_mixed.reshape(text.shape)
    crossed = hidden + project(cross_joined, w_pair[:, width:])
    third, widened, active, output = feedforward_forward(crossed, gains[2], w_up, w_down)
    grad_crossed, g_up, g_down, g_third = feedforward_back(
        cotan, crossed, gains[2], third, widened, active, w_up, w_down
    )
    branch = to_low(grad_crossed)
    g_cross_out = weight_grad(cross_joined, branch)
    grad_cross_joined = to_low(back_project(branch, w_pair[:, width:]))
    grad_query, grad_key, grad_value = attend_backward(
        split_heads(grad_cross_joined),
        cross_soft,
        split_heads(cross_query),
        memory_keys,
        memory_vals,
        cross_mask,
    )
    grad_cross_query = to_low(grad_query.reshape(text.shape))
    mem_shape = (batch, memory.shape[1], width)
    grad_memory = to_low(
        jnp.concatenate([grad_key.reshape(mem_shape), grad_value.reshape(mem_shape)], axis=-1)
    )
    g_cross_query = weight_grad(second, grad_cross_query)
    _, pull = jax.vjp(layer_norm, hidden, gains[1])
    grad_norm, g_second = pull(back_project(grad_cross_query, w_pair[:, :width]))
    grad_hidden = grad_crossed + grad_norm
    grad_text, g_in, g_out, g_first = attention_back(
        grad_hidden,
        text,
        gains[0],
        first,
        queries,
        keys,
        values,
        softmaxed,
        joined,
        self_mask,
        w_in,
        w_out,
    )
    g_pair = jnp.concatenate([g_cross_query, g_cross_out], axis=1)
    return (
        output,
        grad_text,
        grad_memory,
        (g_in, g_out, g_pair, g_up, g_down, jnp.stack([g_first, g_second, g_third])),
    )


def to_whole_images(values, section):
    half = values.shape[0] // 2
    low_part, high_part = values[:half], values[half:]
    incoming = partner(jnp.where(section == 0, high_part, low_part), "section", 0)
    kept = jnp.where(section == 0, low_part, high_part)
    left = jnp.where(section == 0, kept, incoming)
    right = jnp.where(section == 0, incoming, kept)
    return jnp.concatenate([left, right], axis=-1)


def to_half_features(values, section):
    half = values.shape[-1] // 2
    left, right = values[..., :half], values[..., half:]
    incoming = partner(jnp.where(section == 0, right, left), "section", 0)
    kept = jnp.where(section == 0, left, right)
    low_part = jnp.where(section == 0, kept, incoming)
    high_part = jnp.where(section == 0, incoming, kept)
    return jnp.concatenate([low_part, high_part], axis=0)


def gather_blocks(piece, dimension):
    sections = lax.axis_size("section")
    shards = lax.axis_size("dp")
    whole = lax.all_gather(piece[0], ("section", "dp"), axis=0, tiled=False)
    if dimension == 0:
        return whole.reshape(sections, shards * piece.shape[1], piece.shape[2])
    whole = whole.reshape(sections, shards, piece.shape[1], piece.shape[2])
    return whole.transpose(0, 2, 1, 3).reshape(sections, piece.shape[1], -1)


def reduce_blocks(first, second, section, dimension):
    first, second = to_low(first), to_low(second)
    incoming = partner(jnp.where(section == 0, second, first), "section", 0)
    kept = jnp.where(section == 0, first, second)
    total = to_low(kept.astype(jnp.float32) + incoming.astype(jnp.float32))
    share = lax.psum_scatter(total, "dp", scatter_dimension=dimension, tiled=True)
    return lax.psum(share, "rep").astype(jnp.float32)[None]


def local(
    patches,
    captions,
    tissue_keep,
    caption_mask,
    mixing,
    merging,
    crossing,
    widening,
    narrowing,
    scales,
    cotangent,
):
    section = lax.axis_index("section")
    count = patches.shape[1]
    length = captions.shape[1]
    gathered = tuple(
        gather_blocks(piece, dimension)
        for piece, dimension in (
            (mixing, 0),
            (merging, 0),
            (crossing, 0),
            (widening, 0),
            (narrowing, 0),
            (scales, 1),
        )
    )
    enc_weights = tuple(piece[0] for piece in gathered)
    dec_weights = tuple(piece[1] for piece in gathered)
    states = to_whole_images(jnp.concatenate([patches, captions, cotangent], axis=1), section)
    states = states.astype(jnp.float32)
    own_patches = states[:, :count]
    own_text = states[:, count : count + length]
    own_cotan = states[:, count + length :]
    own = own_patches.shape[0]
    keep = lax.dynamic_slice_in_dim(tissue_keep, section * own, own, 0)
    text_keep = lax.dynamic_slice_in_dim(caption_mask, section * own, own, 0)
    memory, saved = encoder_pass(own_patches, keep, enc_weights)
    output, grad_text, grad_memory, dec_grads = decoder_step(
        own_text, text_keep, memory, keep, dec_weights, own_cotan
    )
    grad_patches, enc_grads = encoder_backward(own_patches, saved, enc_weights, grad_memory)
    results = to_half_features(
        jnp.concatenate([to_low(grad_patches), to_low(output), to_low(grad_text)], axis=1),
        section,
    )
    summed = tuple(
        reduce_blocks(first, second, section, dimension)
        for first, second, dimension in zip(enc_grads, dec_grads, (0, 0, 0, 0, 0, 1))
    )
    return (
        results[:, count : count + length],
        results[:, count + length :],
        results[:, :count],
    ) + summed


def solution(mesh):
    in_specs = (
        P(("dp", "rep"), None, "section"),
        P(("dp", "rep"), None, "section"),
        P(("dp", "rep"), None),
        P(("dp", "rep"), None),
        P("section", "dp", None),
        P("section", "dp", None),
        P("section", "dp", None),
        P("section", "dp", None),
        P("section", "dp", None),
        P("section", None, "dp"),
        P(("dp", "rep"), None, "section"),
    )
    out_specs = (
        P(("dp", "rep"), None, "section"),
        P(("dp", "rep"), None, "section"),
        P(("dp", "rep"), None, "section"),
        P("section", "dp", None),
        P("section", "dp", None),
        P("section", "dp", None),
        P("section", "dp", None),
        P("section", "dp", None),
        P("section", None, "dp"),
    )
    return jax.shard_map(local, mesh=mesh, in_specs=in_specs, out_specs=out_specs, check_vma=False)
```

```python
import functools

import jax
import jax.numpy as jnp
from jax import lax
from jax.experimental import pallas as pl
from jax.experimental.pallas import tpu as pltpu
from jax.sharding import PartitionSpec as P

HEADS = 12
MESH_IDS = pl.DeviceIdType.MESH


def partner(value, axis, distance):
    mask = 2**distance
    pairs = [(source, source ^ mask) for source in range(lax.axis_size(axis))]
    return lax.ppermute(value, axis, pairs)


def to_low(values):
    return values.astype(jnp.bfloat16)


def layer_norm(values, gain):
    centered = values - jnp.mean(values, axis=-1, keepdims=True)
    return (
        centered * lax.rsqrt(jnp.mean(centered * centered, axis=-1, keepdims=True) + 1e-05) * gain
    )


def gelu_exact(values):
    return jax.nn.gelu(values, approximate=False)


def project(acts, weight):
    return jnp.einsum("bsd,de->bse", acts, weight, preferred_element_type=jnp.float32)


def back_project(grads, weight):
    return jnp.einsum("bse,de->bsd", grads, weight, preferred_element_type=jnp.float32)


def weight_grad(acts, grads):
    return jnp.einsum("bsd,bse->de", acts, grads, preferred_element_type=jnp.float32)


def split_heads(values):
    return values.reshape(values.shape[0], values.shape[1], HEADS, values.shape[2] // HEADS)


def attend_forward(queries, keys, values, mask):
    scale = queries.shape[-1] ** (-0.5)
    scores = (
        jnp.einsum("bqhe,bkhe->bhqk", queries, keys, preferred_element_type=jnp.float32) * scale
    )
    scores = jnp.where(mask[:, None], scores, -1000000000.0)
    peak = jnp.max(scores, axis=-1, keepdims=True)
    expo = jnp.exp(scores - peak)
    softmaxed = expo / jnp.sum(expo, axis=-1, keepdims=True)
    mixed = jnp.einsum(
        "bhqk,bkhe->bqhe", to_low(softmaxed), values, preferred_element_type=jnp.float32
    )
    return (to_low(mixed), softmaxed)


def attend_backward(grad_mixed, softmaxed, queries, keys, values, mask):
    scale = queries.shape[-1] ** (-0.5)
    grad_soft = jnp.einsum(
        "bqhe,bkhe->bhqk", grad_mixed, values, preferred_element_type=jnp.float32
    )
    grad_value = jnp.einsum(
        "bhqk,bqhe->bkhe", to_low(softmaxed), grad_mixed, preferred_element_type=jnp.float32
    )
    grad_scores = softmaxed * (grad_soft - jnp.sum(softmaxed * grad_soft, axis=-1, keepdims=True))
    grad_scores = to_low(jnp.where(mask[:, None], grad_scores, 0.0))
    grad_query = (
        jnp.einsum("bhqk,bkhe->bqhe", grad_scores, keys, preferred_element_type=jnp.float32) * scale
    )
    grad_key = (
        jnp.einsum("bhqk,bqhe->bkhe", grad_scores, queries, preferred_element_type=jnp.float32)
        * scale
    )
    return (grad_query, grad_key, grad_value)


def attention_forward(states, gain, w_in, w_out, mask):
    width = states.shape[2]
    first = to_low(layer_norm(states, gain))
    united = to_low(project(first, w_in))
    queries = split_heads(united[..., :width])
    keys = split_heads(united[..., width : 2 * width])
    values = split_heads(united[..., 2 * width :])
    mixed, softmaxed = attend_forward(queries, keys, values, mask)
    joined = mixed.reshape(states.shape)
    hidden = states + project(joined, w_out)
    return (first, queries, keys, values, softmaxed, joined, hidden)


def feedforward_forward(states, gain, w_up, w_down):
    second = to_low(layer_norm(states, gain))
    widened = project(second, w_up)
    active = to_low(gelu_exact(widened))
    after = states + project(active, w_down)
    return (second, widened, active, after)


def attention_back(
    grad_after, states, gain, first, queries, keys, values, softmaxed, joined, mask, w_in, w_out
):
    branch = to_low(grad_after)
    g_out = weight_grad(joined, branch)
    grad_joined = to_low(back_project(branch, w_out))
    grad_query, grad_key, grad_value = attend_backward(
        split_heads(grad_joined), softmaxed, queries, keys, values, mask
    )
    shape = states.shape
    grad_united = to_low(
        jnp.concatenate(
            [grad_query.reshape(shape), grad_key.reshape(shape), grad_value.reshape(shape)], axis=-1
        )
    )
    g_in = weight_grad(first, grad_united)
    _, pull = jax.vjp(layer_norm, states, gain)
    grad_norm, g_gain = pull(back_project(grad_united, w_in))
    return (grad_after + grad_norm, g_in, g_out, g_gain)


def feedforward_back(grad_after, states, gain, second, widened, active, w_up, w_down):
    branch = to_low(grad_after)
    g_down = weight_grad(active, branch)
    _, pull = jax.vjp(gelu_exact, widened)
    grad_wide = to_low(pull(back_project(branch, w_down))[0])
    g_up = weight_grad(second, grad_wide)
    _, pull = jax.vjp(layer_norm, states, gain)
    grad_norm, g_gain = pull(back_project(grad_wide, w_up))
    return (grad_after + grad_norm, g_up, g_down, g_gain)


def encoder_pass(states, keep, weights):
    w_in, w_out, w_pair, w_up, w_down, gains = weights
    gains = gains.astype(jnp.float32)
    batch, count, width = states.shape
    mask = jnp.broadcast_to(keep[:, None, :] > 0, (batch, count, count))
    first, queries, keys, values, softmaxed, joined, hidden = attention_forward(
        states, gains[0], w_in, w_out, mask
    )
    second, widened, active, after = feedforward_forward(hidden, gains[1], w_up, w_down)
    final = to_low(layer_norm(after, gains[2]))
    memory = to_low(project(final, w_pair))
    saved = (
        mask,
        first,
        queries,
        keys,
        values,
        softmaxed,
        joined,
        hidden,
        second,
        widened,
        active,
        after,
        final,
    )
    return (memory, saved)


def encoder_backward(states, saved, weights, grad_memory):
    w_in, w_out, w_pair, w_up, w_down, gains = weights
    gains = gains.astype(jnp.float32)
    (
        mask,
        first,
        queries,
        keys,
        values,
        softmaxed,
        joined,
        hidden,
        second,
        widened,
        active,
        after,
        final,
    ) = saved
    g_pair = weight_grad(final, grad_memory)
    _, pull = jax.vjp(layer_norm, after, gains[2])
    grad_after, g_final = pull(back_project(grad_memory, w_pair))
    grad_hidden, g_up, g_down, g_second = feedforward_back(
        grad_after, hidden, gains[1], second, widened, active, w_up, w_down
    )
    grad_states, g_in, g_out, g_first = attention_back(
        grad_hidden,
        states,
        gains[0],
        first,
        queries,
        keys,
        values,
        softmaxed,
        joined,
        mask,
        w_in,
        w_out,
    )
    return (
        grad_states,
        (g_in, g_out, g_pair, g_up, g_down, jnp.stack([g_first, g_second, g_final])),
    )


def decoder_step(text, text_keep, memory, keep, weights, cotan):
    w_in, w_out, w_pair, w_up, w_down, gains = weights
    gains = gains.astype(jnp.float32)
    batch, length, width = text.shape
    query_pos = lax.broadcasted_iota(jnp.int32, (length, length), 0)
    key_pos = lax.broadcasted_iota(jnp.int32, (length, length), 1)
    self_mask = (key_pos <= query_pos)[None] & (text_keep[:, None, :] > 0)
    cross_mask = jnp.broadcast_to(keep[:, None, :] > 0, (batch, length, keep.shape[1]))
    first, queries, keys, values, softmaxed, joined, hidden = attention_forward(
        text, gains[0], w_in, w_out, self_mask
    )
    second = to_low(layer_norm(hidden, gains[1]))
    cross_query = to_low(project(second, w_pair[:, :width]))
    memory_keys = split_heads(memory[..., :width])
    memory_vals = split_heads(memory[..., width:])
    cross_mixed, cross_soft = attend_forward(
        split_heads(cross_query), memory_keys, memory_vals, cross_mask
    )
    cross_joined = cross_mixed.reshape(text.shape)
    crossed = hidden + project(cross_joined, w_pair[:, width:])
    third, widened, active, output = feedforward_forward(crossed, gains[2], w_up, w_down)
    grad_crossed, g_up, g_down, g_third = feedforward_back(
        cotan, crossed, gains[2], third, widened, active, w_up, w_down
    )
    branch = to_low(grad_crossed)
    g_cross_out = weight_grad(cross_joined, branch)
    grad_cross_joined = to_low(back_project(branch, w_pair[:, width:]))
    grad_query, grad_key, grad_value = attend_backward(
        split_heads(grad_cross_joined),
        cross_soft,
        split_heads(cross_query),
        memory_keys,
        memory_vals,
        cross_mask,
    )
    grad_cross_query = to_low(grad_query.reshape(text.shape))
    mem_shape = (batch, memory.shape[1], width)
    grad_memory = to_low(
        jnp.concatenate([grad_key.reshape(mem_shape), grad_value.reshape(mem_shape)], axis=-1)
    )
    g_cross_query = weight_grad(second, grad_cross_query)
    _, pull = jax.vjp(layer_norm, hidden, gains[1])
    grad_norm, g_second = pull(back_project(grad_cross_query, w_pair[:, :width]))
    grad_hidden = grad_crossed + grad_norm
    grad_text, g_in, g_out, g_first = attention_back(
        grad_hidden,
        text,
        gains[0],
        first,
        queries,
        keys,
        values,
        softmaxed,
        joined,
        self_mask,
        w_in,
        w_out,
    )
    g_pair = jnp.concatenate([g_cross_query, g_cross_out], axis=1)
    return (
        output,
        grad_text,
        grad_memory,
        (g_in, g_out, g_pair, g_up, g_down, jnp.stack([g_first, g_second, g_third])),
    )


def to_whole_images(values, section):
    half = values.shape[0] // 2
    low_part, high_part = values[:half], values[half:]
    incoming = partner(jnp.where(section == 0, high_part, low_part), "section", 0)
    kept = jnp.where(section == 0, low_part, high_part)
    left = jnp.where(section == 0, kept, incoming)
    right = jnp.where(section == 0, incoming, kept)
    return jnp.concatenate([left, right], axis=-1)


def to_half_features(values, section):
    half = values.shape[-1] // 2
    left, right = values[..., :half], values[..., half:]
    incoming = partner(jnp.where(section == 0, right, left), "section", 0)
    kept = jnp.where(section == 0, left, right)
    low_part = jnp.where(section == 0, kept, incoming)
    high_part = jnp.where(section == 0, incoming, kept)
    return jnp.concatenate([low_part, high_part], axis=0)


def gather_blocks(piece, dimension):
    sections = lax.axis_size("section")
    shards = lax.axis_size("dp")
    whole = lax.all_gather(piece[0], ("section", "dp"), axis=0, tiled=False)
    if dimension == 0:
        return whole.reshape(sections, shards * piece.shape[1], piece.shape[2])
    whole = whole.reshape(sections, shards, piece.shape[1], piece.shape[2])
    return whole.transpose(0, 2, 1, 3).reshape(sections, piece.shape[1], -1)


def ring_place(shard, size):
    column = shard % 2
    row = shard // 2
    return row * (1 - column) + (size - 1 - row) * column


def ring_shard(place, size):
    column = place // (size // 2)
    row = place * (1 - column) + (size - 1 - place) * column
    return 2 * row + column


def reduce_kernel(size, reps, kinds, *refs):
    grads, outs = refs[:kinds], refs[kinds : 2 * kinds]
    slots, sides = refs[2 * kinds : 3 * kinds], refs[3 * kinds : 4 * kinds]
    send, recv, side_send, side_recv = refs[4 * kinds :]
    place = ring_place(lax.axis_index("dp"), size)
    replica = lax.axis_index("rep")
    targets = (
        ring_shard((place + 1) % size, size),
        ring_shard((place + size - 1) % size, size),
    )
    signs = (-1, 1)

    barrier = pltpu.get_barrier_semaphore()
    for target in targets:
        pl.semaphore_signal(barrier, inc=1, device_id={"dp": target}, device_id_type=MESH_IDS)
    for other in range(1, reps):
        pl.semaphore_signal(
            barrier,
            inc=1,
            device_id={"rep": (replica + other) % reps},
            device_id_type=MESH_IDS,
        )
    pl.semaphore_wait(barrier, 1 + reps)

    def own(kind, way, step):
        chunk = (place + signs[way] * (step + 1) + 2 * size) % size
        return grads[kind].at[ring_shard(chunk, size), way]

    def hop(kind, way, step, source):
        return pltpu.make_async_remote_copy(
            src_ref=source,
            dst_ref=slots[kind].at[step, way],
            send_sem=send.at[kind, way, step],
            recv_sem=recv.at[kind, way, step],
            device_id={"dp": targets[way]},
            device_id_type=MESH_IDS,
        )

    def side(kind, other):
        return pltpu.make_async_remote_copy(
            src_ref=slots[kind].at[size - 2],
            dst_ref=sides[kind].at[other - 1],
            send_sem=side_send.at[kind, other - 1],
            recv_sem=side_recv.at[kind, other - 1],
            device_id={"rep": (replica + other) % reps},
            device_id_type=MESH_IDS,
        )

    def add(kind, way, step):
        slot = slots[kind].at[step, way]
        mine = own(kind, way, step + 1)
        slot[...] = (slot[...].astype(jnp.float32) + mine[...].astype(jnp.float32)).astype(
            jnp.bfloat16
        )

    for kind in range(kinds):
        for way in range(2):
            hop(kind, way, 0, own(kind, way, 0)).start()

    def walk(step, carry):
        for kind in range(kinds):
            for way in range(2):
                hop(kind, way, step, slots[kind].at[step, way]).wait_recv()
                add(kind, way, step)
                hop(kind, way, step + 1, slots[kind].at[step, way]).start()
        return carry

    lax.fori_loop(0, size - 2, walk, 0)
    for kind in range(kinds):
        for way in range(2):
            hop(kind, way, size - 2, slots[kind].at[size - 2, way]).wait_recv()
            add(kind, way, size - 2)
        for other in range(1, reps):
            side(kind, other).start()
    for kind in range(kinds):
        total = slots[kind][size - 2].astype(jnp.float32)
        for other in range(1, reps):
            side(kind, other).wait_recv()
            total += sides[kind][other - 1].astype(jnp.float32)
        outs[kind][...] = total

    def drain(step, carry):
        for kind in range(kinds):
            for way in range(2):
                hop(kind, way, step, slots[kind].at[step, way]).wait_send()
        return carry

    lax.fori_loop(0, size - 1, drain, 0)
    for kind in range(kinds):
        for other in range(1, reps):
            side(kind, other).wait_send()


def reduce_all(grads):
    size, reps = lax.axis_size("dp"), lax.axis_size("rep")
    kinds = len(grads)
    pieces = [g.shape[1:] for g in grads]
    scratch = [pltpu.VMEM((size - 1,) + p, jnp.bfloat16) for p in pieces]
    scratch += [pltpu.VMEM((max(reps - 1, 1),) + p, jnp.bfloat16) for p in pieces]
    scratch += [pltpu.SemaphoreType.DMA((kinds, 2, size - 1))] * 2
    scratch += [pltpu.SemaphoreType.DMA((kinds, max(reps - 1, 1)))] * 2
    return pl.pallas_call(
        functools.partial(reduce_kernel, size, reps, kinds),
        out_shape=[jax.ShapeDtypeStruct(p, jnp.float32) for p in pieces],
        in_specs=[pl.BlockSpec(memory_space=pltpu.VMEM)] * kinds,
        out_specs=[pl.BlockSpec(memory_space=pltpu.VMEM)] * kinds,
        scratch_shapes=scratch,
        compiler_params=pltpu.CompilerParams(
            collective_id=0, has_side_effects=True, vmem_limit_bytes=60 * 1024 * 1024
        ),
    )(*grads)


def by_shard(total, dimension):
    size = lax.axis_size("dp")
    if dimension == 0:
        return total.reshape(size, 2, total.shape[0] // (2 * size), total.shape[1])
    rows, width = total.shape
    part = total.reshape(rows, size, width // size).transpose(1, 0, 2)[:, None]
    return jnp.pad(part, ((0, 0), (0, 1), (0, 16 - rows), (0, 128 - width // size)))


def swap_blocks(first, second, section, dimension):
    first, second = to_low(first), to_low(second)
    incoming = partner(jnp.where(section == 0, second, first), "section", 0)
    kept = jnp.where(section == 0, first, second)
    total = to_low(kept.astype(jnp.float32) + incoming.astype(jnp.float32))
    return by_shard(total, dimension)


def local(
    patches,
    captions,
    tissue_keep,
    caption_mask,
    mixing,
    merging,
    crossing,
    widening,
    narrowing,
    scales,
    cotangent,
):
    section = lax.axis_index("section")
    count = patches.shape[1]
    length = captions.shape[1]
    gathered = tuple(
        gather_blocks(piece, dimension)
        for piece, dimension in (
            (mixing, 0),
            (merging, 0),
            (crossing, 0),
            (widening, 0),
            (narrowing, 0),
            (scales, 1),
        )
    )
    enc_weights = tuple(piece[0] for piece in gathered)
    dec_weights = tuple(piece[1] for piece in gathered)
    states = to_whole_images(jnp.concatenate([patches, captions, cotangent], axis=1), section)
    states = states.astype(jnp.float32)
    own_patches = states[:, :count]
    own_text = states[:, count : count + length]
    own_cotan = states[:, count + length :]
    own = own_patches.shape[0]
    keep = lax.dynamic_slice_in_dim(tissue_keep, section * own, own, 0)
    text_keep = lax.dynamic_slice_in_dim(caption_mask, section * own, own, 0)
    memory, saved = encoder_pass(own_patches, keep, enc_weights)
    output, grad_text, grad_memory, dec_grads = decoder_step(
        own_text, text_keep, memory, keep, dec_weights, own_cotan
    )
    grad_patches, enc_grads = encoder_backward(own_patches, saved, enc_weights, grad_memory)
    results = to_half_features(
        jnp.concatenate([to_low(grad_patches), to_low(output), to_low(grad_text)], axis=1),
        section,
    )
    reduced = reduce_all(
        [
            swap_blocks(first, second, section, dimension)
            for first, second, dimension in zip(enc_grads, dec_grads, (0, 0, 0, 0, 0, 1))
        ]
    )
    summed = tuple(part.reshape(1, -1, part.shape[-1]) for part in reduced[:-1])
    summed += (reduced[-1][:1, : scales.shape[1], : scales.shape[2]],)
    return (
        results[:, count : count + length],
        results[:, count + length :],
        results[:, :count],
    ) + summed


def solution(mesh):
    in_specs = (
        P(("dp", "rep"), None, "section"),
        P(("dp", "rep"), None, "section"),
        P(("dp", "rep"), None),
        P(("dp", "rep"), None),
        P("section", "dp", None),
        P("section", "dp", None),
        P("section", "dp", None),
        P("section", "dp", None),
        P("section", "dp", None),
        P("section", None, "dp"),
        P(("dp", "rep"), None, "section"),
    )
    out_specs = (
        P(("dp", "rep"), None, "section"),
        P(("dp", "rep"), None, "section"),
        P(("dp", "rep"), None, "section"),
        P("section", "dp", None),
        P("section", "dp", None),
        P("section", "dp", None),
        P("section", "dp", None),
        P("section", "dp", None),
        P("section", None, "dp"),
    )
    return jax.shard_map(local, mesh=mesh, in_specs=in_specs, out_specs=out_specs, check_vma=False)
```

```python
import functools

import jax
import jax.numpy as jnp
from jax import lax
from jax.experimental import pallas as pl
from jax.experimental.pallas import tpu as pltpu
from jax.sharding import PartitionSpec as P

HEADS = 12
MESH_IDS = pl.DeviceIdType.MESH


def partner(value, axis, distance):
    mask = 2**distance
    pairs = [(source, source ^ mask) for source in range(lax.axis_size(axis))]
    return lax.ppermute(value, axis, pairs)


def to_low(values):
    return values.astype(jnp.bfloat16)


def layer_norm(values, gain):
    centered = values - jnp.mean(values, axis=-1, keepdims=True)
    return (
        centered * lax.rsqrt(jnp.mean(centered * centered, axis=-1, keepdims=True) + 1e-05) * gain
    )


def gelu_exact(values):
    return jax.nn.gelu(values, approximate=False)


def project(acts, weight):
    return jnp.einsum("bsd,de->bse", acts, weight, preferred_element_type=jnp.float32)


def back_project(grads, weight):
    return jnp.einsum("bse,de->bsd", grads, weight, preferred_element_type=jnp.float32)


def weight_grad(acts, grads):
    return jnp.einsum("bsd,bse->de", acts, grads, preferred_element_type=jnp.float32)


def split_heads(values):
    return values.reshape(values.shape[0], values.shape[1], HEADS, values.shape[2] // HEADS)


def attend_forward(queries, keys, values, mask):
    scale = queries.shape[-1] ** (-0.5)
    scores = (
        jnp.einsum("bqhe,bkhe->bhqk", queries, keys, preferred_element_type=jnp.float32) * scale
    )
    scores = jnp.where(mask[:, None], scores, -1000000000.0)
    peak = jnp.max(scores, axis=-1, keepdims=True)
    expo = jnp.exp(scores - peak)
    softmaxed = expo / jnp.sum(expo, axis=-1, keepdims=True)
    mixed = jnp.einsum(
        "bhqk,bkhe->bqhe", to_low(softmaxed), values, preferred_element_type=jnp.float32
    )
    return (to_low(mixed), softmaxed)


def attend_backward(grad_mixed, softmaxed, queries, keys, values, mask):
    scale = queries.shape[-1] ** (-0.5)
    grad_soft = jnp.einsum(
        "bqhe,bkhe->bhqk", grad_mixed, values, preferred_element_type=jnp.float32
    )
    grad_value = jnp.einsum(
        "bhqk,bqhe->bkhe", to_low(softmaxed), grad_mixed, preferred_element_type=jnp.float32
    )
    grad_scores = softmaxed * (grad_soft - jnp.sum(softmaxed * grad_soft, axis=-1, keepdims=True))
    grad_scores = to_low(jnp.where(mask[:, None], grad_scores, 0.0))
    grad_query = (
        jnp.einsum("bhqk,bkhe->bqhe", grad_scores, keys, preferred_element_type=jnp.float32) * scale
    )
    grad_key = (
        jnp.einsum("bhqk,bqhe->bkhe", grad_scores, queries, preferred_element_type=jnp.float32)
        * scale
    )
    return (grad_query, grad_key, grad_value)


def attention_forward(states, gain, w_in, w_out, mask):
    width = states.shape[2]
    first = to_low(layer_norm(states, gain))
    united = to_low(project(first, w_in))
    queries = split_heads(united[..., :width])
    keys = split_heads(united[..., width : 2 * width])
    values = split_heads(united[..., 2 * width :])
    mixed, softmaxed = attend_forward(queries, keys, values, mask)
    joined = mixed.reshape(states.shape)
    hidden = states + project(joined, w_out)
    return (first, queries, keys, values, softmaxed, joined, hidden)


def feedforward_forward(states, gain, w_up, w_down):
    second = to_low(layer_norm(states, gain))
    widened = project(second, w_up)
    active = to_low(gelu_exact(widened))
    after = states + project(active, w_down)
    return (second, widened, active, after)


def attention_back(
    grad_after, states, gain, first, queries, keys, values, softmaxed, joined, mask, w_in, w_out
):
    branch = to_low(grad_after)
    g_out = weight_grad(joined, branch)
    grad_joined = to_low(back_project(branch, w_out))
    grad_query, grad_key, grad_value = attend_backward(
        split_heads(grad_joined), softmaxed, queries, keys, values, mask
    )
    shape = states.shape
    grad_united = to_low(
        jnp.concatenate(
            [grad_query.reshape(shape), grad_key.reshape(shape), grad_value.reshape(shape)], axis=-1
        )
    )
    g_in = weight_grad(first, grad_united)
    _, pull = jax.vjp(layer_norm, states, gain)
    grad_norm, g_gain = pull(back_project(grad_united, w_in))
    return (grad_after + grad_norm, g_in, g_out, g_gain)


def feedforward_back(grad_after, states, gain, second, widened, active, w_up, w_down):
    branch = to_low(grad_after)
    g_down = weight_grad(active, branch)
    _, pull = jax.vjp(gelu_exact, widened)
    grad_wide = to_low(pull(back_project(branch, w_down))[0])
    g_up = weight_grad(second, grad_wide)
    _, pull = jax.vjp(layer_norm, states, gain)
    grad_norm, g_gain = pull(back_project(grad_wide, w_up))
    return (grad_after + grad_norm, g_up, g_down, g_gain)


def encoder_pass(states, keep, weights):
    w_in, w_out, w_pair, w_up, w_down, gains = weights
    gains = gains.astype(jnp.float32)
    batch, count, width = states.shape
    mask = jnp.broadcast_to(keep[:, None, :] > 0, (batch, count, count))
    first, queries, keys, values, softmaxed, joined, hidden = attention_forward(
        states, gains[0], w_in, w_out, mask
    )
    second, widened, active, after = feedforward_forward(hidden, gains[1], w_up, w_down)
    final = to_low(layer_norm(after, gains[2]))
    memory = to_low(project(final, w_pair))
    saved = (
        mask,
        first,
        queries,
        keys,
        values,
        softmaxed,
        joined,
        hidden,
        second,
        widened,
        active,
        after,
        final,
    )
    return (memory, saved)


def encoder_backward(states, saved, weights, grad_memory):
    w_in, w_out, w_pair, w_up, w_down, gains = weights
    gains = gains.astype(jnp.float32)
    (
        mask,
        first,
        queries,
        keys,
        values,
        softmaxed,
        joined,
        hidden,
        second,
        widened,
        active,
        after,
        final,
    ) = saved
    g_pair = weight_grad(final, grad_memory)
    _, pull = jax.vjp(layer_norm, after, gains[2])
    grad_after, g_final = pull(back_project(grad_memory, w_pair))
    grad_hidden, g_up, g_down, g_second = feedforward_back(
        grad_after, hidden, gains[1], second, widened, active, w_up, w_down
    )
    grad_states, g_in, g_out, g_first = attention_back(
        grad_hidden,
        states,
        gains[0],
        first,
        queries,
        keys,
        values,
        softmaxed,
        joined,
        mask,
        w_in,
        w_out,
    )
    return (
        grad_states,
        (g_in, g_out, g_pair, g_up, g_down, jnp.stack([g_first, g_second, g_final])),
    )


def decoder_step(text, text_keep, memory, keep, weights, cotan):
    w_in, w_out, w_pair, w_up, w_down, gains = weights
    gains = gains.astype(jnp.float32)
    batch, length, width = text.shape
    query_pos = lax.broadcasted_iota(jnp.int32, (length, length), 0)
    key_pos = lax.broadcasted_iota(jnp.int32, (length, length), 1)
    self_mask = (key_pos <= query_pos)[None] & (text_keep[:, None, :] > 0)
    cross_mask = jnp.broadcast_to(keep[:, None, :] > 0, (batch, length, keep.shape[1]))
    first, queries, keys, values, softmaxed, joined, hidden = attention_forward(
        text, gains[0], w_in, w_out, self_mask
    )
    second = to_low(layer_norm(hidden, gains[1]))
    cross_query = to_low(project(second, w_pair[:, :width]))
    memory_keys = split_heads(memory[..., :width])
    memory_vals = split_heads(memory[..., width:])
    cross_mixed, cross_soft = attend_forward(
        split_heads(cross_query), memory_keys, memory_vals, cross_mask
    )
    cross_joined = cross_mixed.reshape(text.shape)
    crossed = hidden + project(cross_joined, w_pair[:, width:])
    third, widened, active, output = feedforward_forward(crossed, gains[2], w_up, w_down)
    grad_crossed, g_up, g_down, g_third = feedforward_back(
        cotan, crossed, gains[2], third, widened, active, w_up, w_down
    )
    branch = to_low(grad_crossed)
    g_cross_out = weight_grad(cross_joined, branch)
    grad_cross_joined = to_low(back_project(branch, w_pair[:, width:]))
    grad_query, grad_key, grad_value = attend_backward(
        split_heads(grad_cross_joined),
        cross_soft,
        split_heads(cross_query),
        memory_keys,
        memory_vals,
        cross_mask,
    )
    grad_cross_query = to_low(grad_query.reshape(text.shape))
    mem_shape = (batch, memory.shape[1], width)
    grad_memory = to_low(
        jnp.concatenate([grad_key.reshape(mem_shape), grad_value.reshape(mem_shape)], axis=-1)
    )
    g_cross_query = weight_grad(second, grad_cross_query)
    _, pull = jax.vjp(layer_norm, hidden, gains[1])
    grad_norm, g_second = pull(back_project(grad_cross_query, w_pair[:, :width]))
    grad_hidden = grad_crossed + grad_norm
    grad_text, g_in, g_out, g_first = attention_back(
        grad_hidden,
        text,
        gains[0],
        first,
        queries,
        keys,
        values,
        softmaxed,
        joined,
        self_mask,
        w_in,
        w_out,
    )
    g_pair = jnp.concatenate([g_cross_query, g_cross_out], axis=1)
    return (
        output,
        grad_text,
        grad_memory,
        (g_in, g_out, g_pair, g_up, g_down, jnp.stack([g_first, g_second, g_third])),
    )


def to_whole_images(values, section):
    half = values.shape[0] // 2
    low_part, high_part = values[:half], values[half:]
    incoming = partner(jnp.where(section == 0, high_part, low_part), "section", 0)
    kept = jnp.where(section == 0, low_part, high_part)
    left = jnp.where(section == 0, kept, incoming)
    right = jnp.where(section == 0, incoming, kept)
    return jnp.concatenate([left, right], axis=-1)


def to_half_features(values, section):
    half = values.shape[-1] // 2
    left, right = values[..., :half], values[..., half:]
    incoming = partner(jnp.where(section == 0, right, left), "section", 0)
    kept = jnp.where(section == 0, left, right)
    low_part = jnp.where(section == 0, kept, incoming)
    high_part = jnp.where(section == 0, incoming, kept)
    return jnp.concatenate([low_part, high_part], axis=0)


def ring_place(shard, size):
    column = shard % 2
    row = shard // 2
    return row * (1 - column) + (size - 1 - row) * column


def ring_shard(place, size):
    column = place // (size // 2)
    row = place * (1 - column) + (size - 1 - place) * column
    return 2 * row + column


def reduce_kernel(size, reps, kinds, *refs):
    grads, outs = refs[:kinds], refs[kinds : 2 * kinds]
    slots, sides = refs[2 * kinds : 3 * kinds], refs[3 * kinds : 4 * kinds]
    send, recv, side_send, side_recv = refs[4 * kinds :]
    place = ring_place(lax.axis_index("dp"), size)
    replica = lax.axis_index("rep")
    targets = (
        ring_shard((place + 1) % size, size),
        ring_shard((place + size - 1) % size, size),
    )
    signs = (-1, 1)

    barrier = pltpu.get_barrier_semaphore()
    for target in targets:
        pl.semaphore_signal(barrier, inc=1, device_id={"dp": target}, device_id_type=MESH_IDS)
    for other in range(1, reps):
        pl.semaphore_signal(
            barrier,
            inc=1,
            device_id={"rep": (replica + other) % reps},
            device_id_type=MESH_IDS,
        )
    pl.semaphore_wait(barrier, 1 + reps)

    def own(kind, way, step):
        chunk = (place + signs[way] * (step + 1) + 2 * size) % size
        return grads[kind].at[ring_shard(chunk, size), way]

    def hop(kind, way, step, source):
        return pltpu.make_async_remote_copy(
            src_ref=source,
            dst_ref=slots[kind].at[step, way],
            send_sem=send.at[kind, way, step],
            recv_sem=recv.at[kind, way, step],
            device_id={"dp": targets[way]},
            device_id_type=MESH_IDS,
        )

    def side(kind, other):
        return pltpu.make_async_remote_copy(
            src_ref=slots[kind].at[size - 2],
            dst_ref=sides[kind].at[other - 1],
            send_sem=side_send.at[kind, other - 1],
            recv_sem=side_recv.at[kind, other - 1],
            device_id={"rep": (replica + other) % reps},
            device_id_type=MESH_IDS,
        )

    def add(kind, way, step):
        slot = slots[kind].at[step, way]
        mine = own(kind, way, step + 1)
        slot[...] = (slot[...].astype(jnp.float32) + mine[...].astype(jnp.float32)).astype(
            jnp.bfloat16
        )

    for kind in range(kinds):
        for way in range(2):
            hop(kind, way, 0, own(kind, way, 0)).start()

    def walk(step, carry):
        for kind in range(kinds):
            for way in range(2):
                hop(kind, way, step, slots[kind].at[step, way]).wait_recv()
                add(kind, way, step)
                hop(kind, way, step + 1, slots[kind].at[step, way]).start()
        return carry

    lax.fori_loop(0, size - 2, walk, 0)
    for kind in range(kinds):
        for way in range(2):
            hop(kind, way, size - 2, slots[kind].at[size - 2, way]).wait_recv()
            add(kind, way, size - 2)
        for other in range(1, reps):
            side(kind, other).start()
    for kind in range(kinds):
        total = slots[kind][size - 2].astype(jnp.float32)
        for other in range(1, reps):
            side(kind, other).wait_recv()
            total += sides[kind][other - 1].astype(jnp.float32)
        outs[kind][...] = total

    def drain(step, carry):
        for kind in range(kinds):
            for way in range(2):
                hop(kind, way, step, slots[kind].at[step, way]).wait_send()
        return carry

    lax.fori_loop(0, size - 1, drain, 0)
    for kind in range(kinds):
        for other in range(1, reps):
            side(kind, other).wait_send()


def reduce_all(grads):
    size, reps = lax.axis_size("dp"), lax.axis_size("rep")
    kinds = len(grads)
    pieces = [g.shape[1:] for g in grads]
    scratch = [pltpu.VMEM((size - 1,) + p, jnp.bfloat16) for p in pieces]
    scratch += [pltpu.VMEM((max(reps - 1, 1),) + p, jnp.bfloat16) for p in pieces]
    scratch += [pltpu.SemaphoreType.DMA((kinds, 2, size - 1))] * 2
    scratch += [pltpu.SemaphoreType.DMA((kinds, max(reps - 1, 1)))] * 2
    return pl.pallas_call(
        functools.partial(reduce_kernel, size, reps, kinds),
        out_shape=[jax.ShapeDtypeStruct(p, jnp.float32) for p in pieces],
        in_specs=[pl.BlockSpec(memory_space=pltpu.VMEM)] * kinds,
        out_specs=[pl.BlockSpec(memory_space=pltpu.VMEM)] * kinds,
        scratch_shapes=scratch,
        compiler_params=pltpu.CompilerParams(
            collective_id=0, has_side_effects=True, vmem_limit_bytes=60 * 1024 * 1024
        ),
    )(*grads)


def by_shard(total, dimension):
    size = lax.axis_size("dp")
    if dimension == 0:
        return total.reshape(size, 2, total.shape[0] // (2 * size), total.shape[1])
    rows, width = total.shape
    part = total.reshape(rows, size, width // size).transpose(1, 0, 2)[:, None]
    return jnp.pad(part, ((0, 0), (0, 1), (0, 16 - rows), (0, 128 - width // size)))


def gather_kernel(size, reps, kinds, cuts, *refs):
    pieces, firsts, seconds = refs[:kinds], refs[kinds : 2 * kinds], refs[2 * kinds : 3 * kinds]
    send, recv, side_send, side_recv, pair_send, pair_recv, keep = refs[3 * kinds :]
    me = lax.axis_index("dp")
    place = ring_place(me, size)
    replica, section = lax.axis_index("rep"), lax.axis_index("section")
    targets = (
        ring_shard((place + 1) % size, size),
        ring_shard((place + size - 1) % size, size),
    )
    signs = (-1, 1)
    helped = [kind for kind in range(kinds) if cuts[kind] > 1]

    barrier = pltpu.get_barrier_semaphore()
    for target in targets:
        pl.semaphore_signal(barrier, inc=1, device_id={"dp": target}, device_id_type=MESH_IDS)
    pl.semaphore_signal(
        barrier, inc=1, device_id={"section": 1 - section}, device_id_type=MESH_IDS
    )
    if helped:
        pl.semaphore_signal(
            barrier, inc=1, device_id={"rep": 1 - replica}, device_id_type=MESH_IDS
        )
    pl.semaphore_wait(barrier, 4 if helped else 3)

    def carry(mine, theirs):
        def holder(way, step):
            return ring_shard((place + signs[way] * step + size) % size, size)

        def ring_rows(kind):
            return pl.ds(replica, 2) if cuts[kind] > 1 else pl.ds(0, 1)

        def hop(kind, way, step, first=False):
            at = holder(way, step)
            source = pieces[kind] if first else mine[kind].at[at]
            return pltpu.make_async_remote_copy(
                src_ref=source.at[way, ring_rows(kind)],
                dst_ref=mine[kind].at[at, way, ring_rows(kind)],
                send_sem=send.at[kind, way, step],
                recv_sem=recv.at[kind, way, step],
                device_id={"dp": targets[way]},
                device_id_type=MESH_IDS,
            )

        def arrived(kind, way, step):
            at = holder(way, step + 1)
            return pltpu.make_async_remote_copy(
                src_ref=mine[kind].at[at, way, ring_rows(kind)],
                dst_ref=mine[kind].at[at, way, ring_rows(kind)],
                send_sem=send.at[kind, way, step],
                recv_sem=recv.at[kind, way, step],
                device_id={"dp": targets[way]},
                device_id_type=MESH_IDS,
            )

        def side(kind, way, step, part):
            region = mine[kind].at[holder(way, step), way, pl.ds(part, 1)]
            return pltpu.make_async_remote_copy(
                src_ref=region,
                dst_ref=region,
                send_sem=side_send.at[kind],
                recv_sem=side_recv.at[kind, way, step - 1],
                device_id={"rep": 1 - replica},
                device_id_type=MESH_IDS,
            )

        def pair(kind, source, target):
            return pltpu.make_async_remote_copy(
                src_ref=source,
                dst_ref=target,
                send_sem=pair_send.at[kind],
                recv_sem=pair_recv.at[kind],
                device_id={"section": 1 - section},
                device_id_type=MESH_IDS,
            )

        def forward(kind, way, step, rows):
            region = mine[kind].at[holder(way, step), way, rows]
            pair(kind, region, region).start()

        def take_side(kind, way, step):
            part = 2 * (1 - replica)
            side(kind, way, step, part).wait_recv()

        for kind in range(kinds):
            for way in range(2):
                hop(kind, way, 0, first=True).start()
        for kind in range(kinds):
            pair(kind, pieces[kind], mine[kind].at[me]).start()
            pltpu.make_async_copy(pieces[kind], mine[kind].at[me], keep.at[kind]).start()

        def settle(step, last=False, sides=True):
            for kind in range(kinds):
                for way in range(2):
                    arrived(kind, way, step).wait_recv()
                    if not last:
                        hop(kind, way, step + 1).start()
                    if cuts[kind] > 1:
                        side(kind, way, step + 1, 2 * replica).start()
                    forward(kind, way, step + 1, ring_rows(kind))
            for kind in helped if sides else []:
                for way in range(2):
                    take_side(kind, way, step)

        def settle_sides(step):
            for kind in helped:
                for way in range(2):
                    forward(kind, way, step, pl.ds(2 * (1 - replica), 1))

        settle(0, sides=False)

        def walk(step, nothing):
            settle(step)
            settle_sides(step)
            return nothing

        lax.fori_loop(1, size - 2, walk, 0)
        settle(size - 2, last=True)
        settle_sides(size - 2)
        for kind in helped:
            for way in range(2):
                take_side(kind, way, size - 1)
        settle_sides(size - 1)

        for kind in range(kinds):
            pltpu.make_async_copy(pieces[kind], mine[kind].at[me], keep.at[kind]).wait()

        def drain(step, nothing):
            for kind in range(kinds):
                for way in range(2):
                    arrived(kind, way, step).wait_send()
            return nothing

        lax.fori_loop(0, size - 1, drain, 0)
        for kind in range(kinds):
            if cuts[kind] > 1:
                sent = mine[kind].at[pl.ds(0, size - 1), :, pl.ds(2 * replica, 1)]
                pltpu.make_async_copy(sent, sent, side_send.at[kind]).wait()
            pltpu.make_async_copy(mine[kind], mine[kind], pair_send.at[kind]).wait()
            pltpu.make_async_copy(theirs[kind], theirs[kind], pair_recv.at[kind]).wait()

    @pl.when(section == 0)
    def _():
        carry(firsts, seconds)

    @pl.when(section == 1)
    def _():
        carry(seconds, firsts)


def cut_of(rows, reps):
    return 3 if reps == 2 and rows % 48 == 0 else 1


def gather_all(pieces):
    size, reps = lax.axis_size("dp"), lax.axis_size("rep")
    kinds = len(pieces)
    cuts = [cut_of(piece.shape[0], reps) for piece in pieces]
    shaped = [
        piece.reshape(2, cut, piece.shape[0] // (2 * cut), piece.shape[1])
        for piece, cut in zip(pieces, cuts)
    ]
    wholes = [jax.ShapeDtypeStruct((size,) + piece.shape, piece.dtype) for piece in shaped]
    scratch = [pltpu.SemaphoreType.DMA((kinds, 2, size - 1))] * 2
    scratch += [pltpu.SemaphoreType.DMA((kinds,)), pltpu.SemaphoreType.DMA((kinds, 2, size - 1))]
    scratch += [pltpu.SemaphoreType.DMA((kinds,))] * 3
    outs = pl.pallas_call(
        functools.partial(gather_kernel, size, reps, kinds, cuts),
        out_shape=wholes * 2,
        in_specs=[pl.BlockSpec(memory_space=pltpu.VMEM)] * kinds,
        out_specs=[pl.BlockSpec(memory_space=pl.ANY)] * (2 * kinds),
        scratch_shapes=scratch,
        compiler_params=pltpu.CompilerParams(collective_id=1, has_side_effects=True),
    )(*shaped)
    return outs[:kinds], outs[kinds:]


def as_weights(outs, rows, width):
    weights = [part.reshape(-1, part.shape[-1]) for part in outs[:-1]]
    gains = outs[-1].reshape(outs[-1].shape[0], -1, outs[-1].shape[-1])[:, :rows, :width]
    return tuple(weights) + (gains.transpose(1, 0, 2).reshape(rows, -1),)


def swap_blocks(first, second, section, dimension):
    first, second = to_low(first), to_low(second)
    incoming = partner(jnp.where(section == 0, second, first), "section", 0)
    kept = jnp.where(section == 0, first, second)
    total = to_low(kept.astype(jnp.float32) + incoming.astype(jnp.float32))
    return by_shard(total, dimension)


def local(
    patches,
    captions,
    tissue_keep,
    caption_mask,
    mixing,
    merging,
    crossing,
    widening,
    narrowing,
    scales,
    cotangent,
):
    section = lax.axis_index("section")
    count = patches.shape[1]
    length = captions.shape[1]
    rows, width = scales.shape[1:]
    gains = jnp.pad(scales[0], ((0, 48 - rows), (0, 128 - width)))
    firsts, seconds = gather_all(
        [mixing[0], merging[0], crossing[0], widening[0], narrowing[0], gains]
    )
    enc_weights = as_weights(firsts, rows, width)
    dec_weights = as_weights(seconds, rows, width)
    states = to_whole_images(jnp.concatenate([patches, captions, cotangent], axis=1), section)
    states = states.astype(jnp.float32)
    own_patches = states[:, :count]
    own_text = states[:, count : count + length]
    own_cotan = states[:, count + length :]
    own = own_patches.shape[0]
    keep = lax.dynamic_slice_in_dim(tissue_keep, section * own, own, 0)
    text_keep = lax.dynamic_slice_in_dim(caption_mask, section * own, own, 0)
    memory, saved = encoder_pass(own_patches, keep, enc_weights)
    output, grad_text, grad_memory, dec_grads = decoder_step(
        own_text, text_keep, memory, keep, dec_weights, own_cotan
    )
    grad_patches, enc_grads = encoder_backward(own_patches, saved, enc_weights, grad_memory)
    results = to_half_features(
        jnp.concatenate([to_low(grad_patches), to_low(output), to_low(grad_text)], axis=1),
        section,
    )
    reduced = reduce_all(
        [
            swap_blocks(first, second, section, dimension)
            for first, second, dimension in zip(enc_grads, dec_grads, (0, 0, 0, 0, 0, 1))
        ]
    )
    summed = tuple(part.reshape(1, -1, part.shape[-1]) for part in reduced[:-1])
    summed += (reduced[-1][:1, :rows, :width],)
    return (
        results[:, count : count + length],
        results[:, count + length :],
        results[:, :count],
    ) + summed


def solution(mesh):
    in_specs = (
        P(("dp", "rep"), None, "section"),
        P(("dp", "rep"), None, "section"),
        P(("dp", "rep"), None),
        P(("dp", "rep"), None),
        P("section", "dp", None),
        P("section", "dp", None),
        P("section", "dp", None),
        P("section", "dp", None),
        P("section", "dp", None),
        P("section", None, "dp"),
        P(("dp", "rep"), None, "section"),
    )
    out_specs = (
        P(("dp", "rep"), None, "section"),
        P(("dp", "rep"), None, "section"),
        P(("dp", "rep"), None, "section"),
        P("section", "dp", None),
        P("section", "dp", None),
        P("section", "dp", None),
        P("section", "dp", None),
        P("section", "dp", None),
        P("section", None, "dp"),
    )
    return jax.shard_map(local, mesh=mesh, in_specs=in_specs, out_specs=out_specs, check_vma=False)
```

```python
import functools

import jax
import jax.numpy as jnp
from jax import lax
from jax.experimental import pallas as pl
from jax.experimental.pallas import tpu as pltpu
from jax.sharding import PartitionSpec as P

HEADS = 12
MESH_IDS = pl.DeviceIdType.MESH


def partner(value, axis, distance):
    mask = 2**distance
    pairs = [(source, source ^ mask) for source in range(lax.axis_size(axis))]
    return lax.ppermute(value, axis, pairs)


def to_low(values):
    return values.astype(jnp.bfloat16)


def layer_norm(values, gain):
    centered = values - jnp.mean(values, axis=-1, keepdims=True)
    return (
        centered * lax.rsqrt(jnp.mean(centered * centered, axis=-1, keepdims=True) + 1e-05) * gain
    )


def gelu_exact(values):
    return jax.nn.gelu(values, approximate=False)


def project(acts, weight):
    return jnp.einsum("bsd,de->bse", acts, weight, preferred_element_type=jnp.float32)


def back_project(grads, weight):
    return jnp.einsum("bse,de->bsd", grads, weight, preferred_element_type=jnp.float32)


def weight_grad(acts, grads):
    return jnp.einsum("bsd,bse->de", acts, grads, preferred_element_type=jnp.float32)


def across(left, right):
    return lax.dot_general(left, right, (((1,), (1,)), ((), ())), preferred_element_type=jnp.float32)


def along(left, right):
    return lax.dot_general(left, right, (((0,), (0,)), ((), ())), preferred_element_type=jnp.float32)


def plain(left, right):
    return lax.dot_general(left, right, (((1,), (0,)), ((), ())), preferred_element_type=jnp.float32)


def seen_keys(keep, keys, queries, causal):
    seen = jnp.broadcast_to(keep > 0, (keys, queries))
    if causal:
        key_at = lax.broadcasted_iota(jnp.int32, (keys, queries), 0)
        query_at = lax.broadcasted_iota(jnp.int32, (keys, queries), 1)
        seen = seen & (key_at <= query_at)
    return seen


def soft_keys(keys, queries, seen, scale):
    scores = jnp.where(seen, across(keys, queries) * scale, -1000000000.0)
    expo = jnp.exp(scores - jnp.max(scores, axis=0, keepdims=True))
    return expo * (1.0 / jnp.sum(expo, axis=0, keepdims=True))


def halves_of(values):
    lane = lax.broadcasted_iota(jnp.int32, values.shape, 1)
    in_first = lane < values.shape[1] // 2
    zero = jnp.zeros_like(values)
    return (jnp.where(in_first, values, zero), jnp.where(in_first, zero, values))


def join_halves(first, second):
    lane = lax.broadcasted_iota(jnp.int32, first.shape, 1)
    return jnp.where(lane < first.shape[1] // 2, first, second)


def attend_kernel(causal, width, joint, scale, *refs):
    if joint:
        q_ref, keep_ref, out_ref = refs
        k_ref, key_at, value_at = q_ref, width, 2 * width
    else:
        q_ref, k_ref, keep_ref, out_ref = refs
        key_at, value_at = 0, width
    count, length = k_ref.shape[1], q_ref.shape[1]
    seen = seen_keys(keep_ref[0], count, length, causal)
    pair = 2 * width // HEADS
    for at in range(0, width, pair):
        queries = q_ref[0, :, at : at + pair]
        values = k_ref[0, :, value_at + at : value_at + at + pair]
        mixed = [
            along(to_low(soft_keys(keys, queries, seen, scale)), values)
            for keys in halves_of(k_ref[0, :, key_at + at : key_at + at + pair])
        ]
        out_ref[0, :, at : at + pair] = to_low(join_halves(*mixed))


def attend_back_kernel(causal, width, joint, scale, *refs):
    if joint:
        q_ref, keep_ref, g_ref, dq_ref = refs
        k_ref, dk_ref, key_at, value_at = q_ref, dq_ref, width, 2 * width
    else:
        q_ref, k_ref, keep_ref, g_ref, dq_ref, dk_ref = refs
        key_at, value_at = 0, width
    count, length = k_ref.shape[1], q_ref.shape[1]
    seen = seen_keys(keep_ref[0], count, length, causal)
    pair = 2 * width // HEADS
    for at in range(0, width, pair):
        queries = q_ref[0, :, at : at + pair]
        grads = g_ref[0, :, at : at + pair]
        all_keys = k_ref[0, :, key_at + at : key_at + at + pair]
        all_values = k_ref[0, :, value_at + at : value_at + at + pair]
        parts = []
        for keys, values in zip(halves_of(all_keys), halves_of(all_values)):
            soft = soft_keys(keys, queries, seen, scale)
            grad_soft = across(values, grads)
            inner = jnp.sum(soft * grad_soft, axis=0, keepdims=True)
            grad_scores = to_low(jnp.where(seen, soft * (grad_soft - inner), 0.0))
            parts.append(
                (
                    along(grad_scores, all_keys) * scale,
                    plain(grad_scores, queries) * scale,
                    plain(to_low(soft), grads),
                )
            )
        grad_query, grad_key, grad_value = (join_halves(*both) for both in zip(*parts))
        dq_ref[0, :, at : at + pair] = to_low(grad_query)
        dk_ref[0, :, key_at + at : key_at + at + pair] = to_low(grad_key)
        dk_ref[0, :, value_at + at : value_at + at + pair] = to_low(grad_value)


def per_image(value):
    return pl.BlockSpec((1,) + value.shape[1:], lambda image: (image, 0, 0))


def attend(queries, memory, keep, causal):
    joint = memory is None
    width = queries.shape[2] // 3 if joint else queries.shape[2]
    operands = [queries] if joint else [queries, memory]
    operands.append(keep[:, :, None])
    out = jax.ShapeDtypeStruct(queries.shape[:2] + (width,), jnp.bfloat16)
    scale = (width // HEADS) ** (-0.5)
    return pl.pallas_call(
        functools.partial(attend_kernel, causal, width, joint, scale),
        grid=(queries.shape[0],),
        out_shape=out,
        in_specs=[per_image(value) for value in operands],
        out_specs=per_image(out),
    )(*operands)


def attend_back(grad_mixed, queries, memory, keep, causal):
    joint = memory is None
    width = grad_mixed.shape[2]
    operands = [queries] if joint else [queries, memory]
    outs = [jax.ShapeDtypeStruct(value.shape, jnp.bfloat16) for value in operands]
    operands += [keep[:, :, None], grad_mixed]
    scale = (width // HEADS) ** (-0.5)
    return pl.pallas_call(
        functools.partial(attend_back_kernel, causal, width, joint, scale),
        grid=(queries.shape[0],),
        out_shape=outs,
        in_specs=[per_image(value) for value in operands],
        out_specs=[per_image(value) for value in outs],
    )(*operands)


def attention_forward(states, gain, w_in, w_out, keep, causal):
    first = to_low(layer_norm(states, gain))
    united = to_low(project(first, w_in))
    joined = attend(united, None, keep, causal)
    hidden = states + project(joined, w_out)
    return (first, united, joined, hidden)


def feedforward_forward(states, gain, w_up, w_down):
    second = to_low(layer_norm(states, gain))
    widened = project(second, w_up)
    active = to_low(gelu_exact(widened))
    after = states + project(active, w_down)
    return (second, widened, active, after)


def attention_back(grad_after, states, gain, first, united, joined, keep, causal, w_in, w_out):
    branch = to_low(grad_after)
    g_out = weight_grad(joined, branch)
    grad_joined = to_low(back_project(branch, w_out))
    (grad_united,) = attend_back(grad_joined, united, None, keep, causal)
    g_in = weight_grad(first, grad_united)
    _, pull = jax.vjp(layer_norm, states, gain)
    grad_norm, g_gain = pull(back_project(grad_united, w_in))
    return (grad_after + grad_norm, g_in, g_out, g_gain)


def feedforward_back(grad_after, states, gain, second, widened, active, w_up, w_down):
    branch = to_low(grad_after)
    g_down = weight_grad(active, branch)
    _, pull = jax.vjp(gelu_exact, widened)
    grad_wide = to_low(pull(back_project(branch, w_down))[0])
    g_up = weight_grad(second, grad_wide)
    _, pull = jax.vjp(layer_norm, states, gain)
    grad_norm, g_gain = pull(back_project(grad_wide, w_up))
    return (grad_after + grad_norm, g_up, g_down, g_gain)


def encoder_pass(states, keep, weights):
    w_in, w_out, w_pair, w_up, w_down, gains = weights
    gains = gains.astype(jnp.float32)
    first, united, joined, hidden = attention_forward(
        states, gains[0], w_in, w_out, keep, False
    )
    second, widened, active, after = feedforward_forward(hidden, gains[1], w_up, w_down)
    final = to_low(layer_norm(after, gains[2]))
    memory = to_low(project(final, w_pair))
    return (memory, (first, united, joined, hidden, second, widened, active, after, final))


def encoder_backward(states, keep, saved, weights, grad_memory):
    w_in, w_out, w_pair, w_up, w_down, gains = weights
    gains = gains.astype(jnp.float32)
    first, united, joined, hidden, second, widened, active, after, final = saved
    g_pair = weight_grad(final, grad_memory)
    _, pull = jax.vjp(layer_norm, after, gains[2])
    grad_after, g_final = pull(back_project(grad_memory, w_pair))
    grad_hidden, g_up, g_down, g_second = feedforward_back(
        grad_after, hidden, gains[1], second, widened, active, w_up, w_down
    )
    grad_states, g_in, g_out, g_first = attention_back(
        grad_hidden, states, gains[0], first, united, joined, keep, False, w_in, w_out
    )
    return (
        grad_states,
        (g_in, g_out, g_pair, g_up, g_down, jnp.stack([g_first, g_second, g_final])),
    )


def decoder_step(text, text_keep, memory, keep, weights, cotan):
    w_in, w_out, w_pair, w_up, w_down, gains = weights
    gains = gains.astype(jnp.float32)
    width = text.shape[2]
    first, united, joined, hidden = attention_forward(
        text, gains[0], w_in, w_out, text_keep, True
    )
    second = to_low(layer_norm(hidden, gains[1]))
    cross_query = to_low(project(second, w_pair[:, :width]))
    cross_joined = attend(cross_query, memory, keep, False)
    crossed = hidden + project(cross_joined, w_pair[:, width:])
    third, widened, active, output = feedforward_forward(crossed, gains[2], w_up, w_down)
    grad_crossed, g_up, g_down, g_third = feedforward_back(
        cotan, crossed, gains[2], third, widened, active, w_up, w_down
    )
    branch = to_low(grad_crossed)
    g_cross_out = weight_grad(cross_joined, branch)
    grad_cross_joined = to_low(back_project(branch, w_pair[:, width:]))
    grad_cross_query, grad_memory = attend_back(
        grad_cross_joined, cross_query, memory, keep, False
    )
    g_cross_query = weight_grad(second, grad_cross_query)
    _, pull = jax.vjp(layer_norm, hidden, gains[1])
    grad_norm, g_second = pull(back_project(grad_cross_query, w_pair[:, :width]))
    grad_hidden = grad_crossed + grad_norm
    grad_text, g_in, g_out, g_first = attention_back(
        grad_hidden, text, gains[0], first, united, joined, text_keep, True, w_in, w_out
    )
    g_pair = jnp.concatenate([g_cross_query, g_cross_out], axis=1)
    return (
        output,
        grad_text,
        grad_memory,
        (g_in, g_out, g_pair, g_up, g_down, jnp.stack([g_first, g_second, g_third])),
    )


def to_whole_images(values, section):
    half = values.shape[0] // 2
    low_part, high_part = values[:half], values[half:]
    incoming = partner(jnp.where(section == 0, high_part, low_part), "section", 0)
    kept = jnp.where(section == 0, low_part, high_part)
    left = jnp.where(section == 0, kept, incoming)
    right = jnp.where(section == 0, incoming, kept)
    return jnp.concatenate([left, right], axis=-1)


def to_half_features(values, section):
    half = values.shape[-1] // 2
    left, right = values[..., :half], values[..., half:]
    incoming = partner(jnp.where(section == 0, right, left), "section", 0)
    kept = jnp.where(section == 0, left, right)
    low_part = jnp.where(section == 0, kept, incoming)
    high_part = jnp.where(section == 0, incoming, kept)
    return jnp.concatenate([low_part, high_part], axis=0)


def ring_place(shard, size):
    column = shard % 2
    row = shard // 2
    return row * (1 - column) + (size - 1 - row) * column


def ring_shard(place, size):
    column = place // (size // 2)
    row = place * (1 - column) + (size - 1 - place) * column
    return 2 * row + column


def reduce_kernel(size, reps, kinds, *refs):
    grads, outs = refs[:kinds], refs[kinds : 2 * kinds]
    slots, sides = refs[2 * kinds : 3 * kinds], refs[3 * kinds : 4 * kinds]
    send, recv, side_send, side_recv = refs[4 * kinds :]
    place = ring_place(lax.axis_index("dp"), size)
    replica = lax.axis_index("rep")
    targets = (
        ring_shard((place + 1) % size, size),
        ring_shard((place + size - 1) % size, size),
    )
    signs = (-1, 1)

    barrier = pltpu.get_barrier_semaphore()
    for target in targets:
        pl.semaphore_signal(barrier, inc=1, device_id={"dp": target}, device_id_type=MESH_IDS)
    for other in range(1, reps):
        pl.semaphore_signal(
            barrier,
            inc=1,
            device_id={"rep": (replica + other) % reps},
            device_id_type=MESH_IDS,
        )
    pl.semaphore_wait(barrier, 1 + reps)

    def own(kind, way, step):
        chunk = (place + signs[way] * (step + 1) + 2 * size) % size
        return grads[kind].at[ring_shard(chunk, size), way]

    def hop(kind, way, step, source):
        return pltpu.make_async_remote_copy(
            src_ref=source,
            dst_ref=slots[kind].at[step, way],
            send_sem=send.at[kind, way, step],
            recv_sem=recv.at[kind, way, step],
            device_id={"dp": targets[way]},
            device_id_type=MESH_IDS,
        )

    def side(kind, other):
        return pltpu.make_async_remote_copy(
            src_ref=slots[kind].at[size - 2],
            dst_ref=sides[kind].at[other - 1],
            send_sem=side_send.at[kind, other - 1],
            recv_sem=side_recv.at[kind, other - 1],
            device_id={"rep": (replica + other) % reps},
            device_id_type=MESH_IDS,
        )

    def add(kind, way, step):
        slot = slots[kind].at[step, way]
        mine = own(kind, way, step + 1)
        slot[...] = (slot[...].astype(jnp.float32) + mine[...].astype(jnp.float32)).astype(
            jnp.bfloat16
        )

    for kind in range(kinds):
        for way in range(2):
            hop(kind, way, 0, own(kind, way, 0)).start()

    def walk(step, carry):
        for kind in range(kinds):
            for way in range(2):
                hop(kind, way, step, slots[kind].at[step, way]).wait_recv()
                add(kind, way, step)
                hop(kind, way, step + 1, slots[kind].at[step, way]).start()
        return carry

    lax.fori_loop(0, size - 2, walk, 0)
    for kind in range(kinds):
        for way in range(2):
            hop(kind, way, size - 2, slots[kind].at[size - 2, way]).wait_recv()
            add(kind, way, size - 2)
        for other in range(1, reps):
            side(kind, other).start()
    for kind in range(kinds):
        total = slots[kind][size - 2].astype(jnp.float32)
        for other in range(1, reps):
            side(kind, other).wait_recv()
            total += sides[kind][other - 1].astype(jnp.float32)
        outs[kind][...] = total

    def drain(step, carry):
        for kind in range(kinds):
            for way in range(2):
                hop(kind, way, step, slots[kind].at[step, way]).wait_send()
        return carry

    lax.fori_loop(0, size - 1, drain, 0)
    for kind in range(kinds):
        for other in range(1, reps):
            side(kind, other).wait_send()


def reduce_all(grads):
    size, reps = lax.axis_size("dp"), lax.axis_size("rep")
    kinds = len(grads)
    pieces = [g.shape[1:] for g in grads]
    scratch = [pltpu.VMEM((size - 1,) + p, jnp.bfloat16) for p in pieces]
    scratch += [pltpu.VMEM((max(reps - 1, 1),) + p, jnp.bfloat16) for p in pieces]
    scratch += [pltpu.SemaphoreType.DMA((kinds, 2, size - 1))] * 2
    scratch += [pltpu.SemaphoreType.DMA((kinds, max(reps - 1, 1)))] * 2
    return pl.pallas_call(
        functools.partial(reduce_kernel, size, reps, kinds),
        out_shape=[jax.ShapeDtypeStruct(p, jnp.float32) for p in pieces],
        in_specs=[pl.BlockSpec(memory_space=pltpu.VMEM)] * kinds,
        out_specs=[pl.BlockSpec(memory_space=pltpu.VMEM)] * kinds,
        scratch_shapes=scratch,
        compiler_params=pltpu.CompilerParams(
            collective_id=0, has_side_effects=True, vmem_limit_bytes=60 * 1024 * 1024
        ),
    )(*grads)


def by_shard(total, dimension):
    size = lax.axis_size("dp")
    if dimension == 0:
        return total.reshape(size, 2, total.shape[0] // (2 * size), total.shape[1])
    rows, width = total.shape
    part = total.reshape(rows, size, width // size).transpose(1, 0, 2)[:, None]
    return jnp.pad(part, ((0, 0), (0, 1), (0, 16 - rows), (0, 128 - width // size)))


def gather_kernel(size, reps, kinds, cuts, *refs):
    pieces, firsts, seconds = refs[:kinds], refs[kinds : 2 * kinds], refs[2 * kinds : 3 * kinds]
    send, recv, side_send, side_recv, pair_send, pair_recv, keep = refs[3 * kinds :]
    me = lax.axis_index("dp")
    place = ring_place(me, size)
    replica, section = lax.axis_index("rep"), lax.axis_index("section")
    targets = (
        ring_shard((place + 1) % size, size),
        ring_shard((place + size - 1) % size, size),
    )
    signs = (-1, 1)
    helped = [kind for kind in range(kinds) if cuts[kind] > 1]

    barrier = pltpu.get_barrier_semaphore()
    for target in targets:
        pl.semaphore_signal(barrier, inc=1, device_id={"dp": target}, device_id_type=MESH_IDS)
    pl.semaphore_signal(
        barrier, inc=1, device_id={"section": 1 - section}, device_id_type=MESH_IDS
    )
    if helped:
        pl.semaphore_signal(
            barrier, inc=1, device_id={"rep": 1 - replica}, device_id_type=MESH_IDS
        )
    pl.semaphore_wait(barrier, 4 if helped else 3)

    def carry(mine, theirs):
        def holder(way, step):
            return ring_shard((place + signs[way] * step + size) % size, size)

        def ring_rows(kind):
            return pl.ds(replica, 2) if cuts[kind] > 1 else pl.ds(0, 1)

        def hop(kind, way, step, first=False):
            at = holder(way, step)
            source = pieces[kind] if first else mine[kind].at[at]
            return pltpu.make_async_remote_copy(
                src_ref=source.at[way, ring_rows(kind)],
                dst_ref=mine[kind].at[at, way, ring_rows(kind)],
                send_sem=send.at[kind, way, step],
                recv_sem=recv.at[kind, way, step],
                device_id={"dp": targets[way]},
                device_id_type=MESH_IDS,
            )

        def arrived(kind, way, step):
            at = holder(way, step + 1)
            return pltpu.make_async_remote_copy(
                src_ref=mine[kind].at[at, way, ring_rows(kind)],
                dst_ref=mine[kind].at[at, way, ring_rows(kind)],
                send_sem=send.at[kind, way, step],
                recv_sem=recv.at[kind, way, step],
                device_id={"dp": targets[way]},
                device_id_type=MESH_IDS,
            )

        def side(kind, way, step, part):
            region = mine[kind].at[holder(way, step), way, pl.ds(part, 1)]
            return pltpu.make_async_remote_copy(
                src_ref=region,
                dst_ref=region,
                send_sem=side_send.at[kind],
                recv_sem=side_recv.at[kind, way, step - 1],
                device_id={"rep": 1 - replica},
                device_id_type=MESH_IDS,
            )

        def pair(kind, source, target):
            return pltpu.make_async_remote_copy(
                src_ref=source,
                dst_ref=target,
                send_sem=pair_send.at[kind],
                recv_sem=pair_recv.at[kind],
                device_id={"section": 1 - section},
                device_id_type=MESH_IDS,
            )

        def forward(kind, way, step, rows):
            region = mine[kind].at[holder(way, step), way, rows]
            pair(kind, region, region).start()

        def take_side(kind, way, step):
            part = 2 * (1 - replica)
            side(kind, way, step, part).wait_recv()

        for kind in range(kinds):
            for way in range(2):
                hop(kind, way, 0, first=True).start()
        for kind in range(kinds):
            pair(kind, pieces[kind], mine[kind].at[me]).start()
            pltpu.make_async_copy(pieces[kind], mine[kind].at[me], keep.at[kind]).start()

        def settle(step, last=False, sides=True):
            for kind in range(kinds):
                for way in range(2):
                    arrived(kind, way, step).wait_recv()
                    if not last:
                        hop(kind, way, step + 1).start()
                    if cuts[kind] > 1:
                        side(kind, way, step + 1, 2 * replica).start()
                    forward(kind, way, step + 1, ring_rows(kind))
            for kind in helped if sides else []:
                for way in range(2):
                    take_side(kind, way, step)

        def settle_sides(step):
            for kind in helped:
                for way in range(2):
                    forward(kind, way, step, pl.ds(2 * (1 - replica), 1))

        settle(0, sides=False)

        def walk(step, nothing):
            settle(step)
            settle_sides(step)
            return nothing

        lax.fori_loop(1, size - 2, walk, 0)
        settle(size - 2, last=True)
        settle_sides(size - 2)
        for kind in helped:
            for way in range(2):
                take_side(kind, way, size - 1)
        settle_sides(size - 1)

        for kind in range(kinds):
            pltpu.make_async_copy(pieces[kind], mine[kind].at[me], keep.at[kind]).wait()

        def drain(step, nothing):
            for kind in range(kinds):
                for way in range(2):
                    arrived(kind, way, step).wait_send()
            return nothing

        lax.fori_loop(0, size - 1, drain, 0)
        for kind in range(kinds):
            if cuts[kind] > 1:
                sent = mine[kind].at[pl.ds(0, size - 1), :, pl.ds(2 * replica, 1)]
                pltpu.make_async_copy(sent, sent, side_send.at[kind]).wait()
            pltpu.make_async_copy(mine[kind], mine[kind], pair_send.at[kind]).wait()
            pltpu.make_async_copy(theirs[kind], theirs[kind], pair_recv.at[kind]).wait()

    @pl.when(section == 0)
    def _():
        carry(firsts, seconds)

    @pl.when(section == 1)
    def _():
        carry(seconds, firsts)


def cut_of(rows, reps):
    return 3 if reps == 2 and rows % 48 == 0 else 1


def gather_all(pieces):
    size, reps = lax.axis_size("dp"), lax.axis_size("rep")
    kinds = len(pieces)
    cuts = [cut_of(piece.shape[0], reps) for piece in pieces]
    shaped = [
        piece.reshape(2, cut, piece.shape[0] // (2 * cut), piece.shape[1])
        for piece, cut in zip(pieces, cuts)
    ]
    wholes = [jax.ShapeDtypeStruct((size,) + piece.shape, piece.dtype) for piece in shaped]
    scratch = [pltpu.SemaphoreType.DMA((kinds, 2, size - 1))] * 2
    scratch += [pltpu.SemaphoreType.DMA((kinds,)), pltpu.SemaphoreType.DMA((kinds, 2, size - 1))]
    scratch += [pltpu.SemaphoreType.DMA((kinds,))] * 3
    outs = pl.pallas_call(
        functools.partial(gather_kernel, size, reps, kinds, cuts),
        out_shape=wholes * 2,
        in_specs=[pl.BlockSpec(memory_space=pltpu.VMEM)] * kinds,
        out_specs=[pl.BlockSpec(memory_space=pl.ANY)] * (2 * kinds),
        scratch_shapes=scratch,
        compiler_params=pltpu.CompilerParams(collective_id=1, has_side_effects=True),
    )(*shaped)
    return outs[:kinds], outs[kinds:]


def as_weights(outs, rows, width):
    weights = [part.reshape(-1, part.shape[-1]) for part in outs[:-1]]
    gains = outs[-1].reshape(outs[-1].shape[0], -1, outs[-1].shape[-1])[:, :rows, :width]
    return tuple(weights) + (gains.transpose(1, 0, 2).reshape(rows, -1),)


def swap_blocks(first, second, section, dimension):
    first, second = to_low(first), to_low(second)
    incoming = partner(jnp.where(section == 0, second, first), "section", 0)
    kept = jnp.where(section == 0, first, second)
    total = to_low(kept.astype(jnp.float32) + incoming.astype(jnp.float32))
    return by_shard(total, dimension)


def local(
    patches,
    captions,
    tissue_keep,
    caption_mask,
    mixing,
    merging,
    crossing,
    widening,
    narrowing,
    scales,
    cotangent,
):
    section = lax.axis_index("section")
    count = patches.shape[1]
    length = captions.shape[1]
    rows, width = scales.shape[1:]
    gains = jnp.pad(scales[0], ((0, 48 - rows), (0, 128 - width)))
    firsts, seconds = gather_all(
        [mixing[0], merging[0], crossing[0], widening[0], narrowing[0], gains]
    )
    enc_weights = as_weights(firsts, rows, width)
    dec_weights = as_weights(seconds, rows, width)
    states = to_whole_images(jnp.concatenate([patches, captions, cotangent], axis=1), section)
    states = states.astype(jnp.float32)
    own_patches = states[:, :count]
    own_text = states[:, count : count + length]
    own_cotan = states[:, count + length :]
    own = own_patches.shape[0]
    keep = lax.dynamic_slice_in_dim(tissue_keep, section * own, own, 0)
    text_keep = lax.dynamic_slice_in_dim(caption_mask, section * own, own, 0)
    memory, saved = encoder_pass(own_patches, keep, enc_weights)
    output, grad_text, grad_memory, dec_grads = decoder_step(
        own_text, text_keep, memory, keep, dec_weights, own_cotan
    )
    grad_patches, enc_grads = encoder_backward(
        own_patches, keep, saved, enc_weights, grad_memory
    )
    results = to_half_features(
        jnp.concatenate([to_low(grad_patches), to_low(output), to_low(grad_text)], axis=1),
        section,
    )
    reduced = reduce_all(
        [
            swap_blocks(first, second, section, dimension)
            for first, second, dimension in zip(enc_grads, dec_grads, (0, 0, 0, 0, 0, 1))
        ]
    )
    summed = tuple(part.reshape(1, -1, part.shape[-1]) for part in reduced[:-1])
    summed += (reduced[-1][:1, :rows, :width],)
    return (
        results[:, count : count + length],
        results[:, count + length :],
        results[:, :count],
    ) + summed


def solution(mesh):
    in_specs = (
        P(("dp", "rep"), None, "section"),
        P(("dp", "rep"), None, "section"),
        P(("dp", "rep"), None),
        P(("dp", "rep"), None),
        P("section", "dp", None),
        P("section", "dp", None),
        P("section", "dp", None),
        P("section", "dp", None),
        P("section", "dp", None),
        P("section", None, "dp"),
        P(("dp", "rep"), None, "section"),
    )
    out_specs = (
        P(("dp", "rep"), None, "section"),
        P(("dp", "rep"), None, "section"),
        P(("dp", "rep"), None, "section"),
        P("section", "dp", None),
        P("section", "dp", None),
        P("section", "dp", None),
        P("section", "dp", None),
        P("section", "dp", None),
        P("section", None, "dp"),
    )
    return jax.shard_map(local, mesh=mesh, in_specs=in_specs, out_specs=out_specs, check_vma=False)
```

```python
import functools

import jax
import jax.numpy as jnp
from jax import lax
from jax.experimental import pallas as pl
from jax.experimental.pallas import tpu as pltpu
from jax.sharding import PartitionSpec as P

HEADS = 12
MESH_IDS = pl.DeviceIdType.MESH


def partner(value, axis, distance):
    mask = 2**distance
    pairs = [(source, source ^ mask) for source in range(lax.axis_size(axis))]
    return lax.ppermute(value, axis, pairs)


def to_low(values):
    return values.astype(jnp.bfloat16)


def layer_norm(values, gain):
    centered = values - jnp.mean(values, axis=-1, keepdims=True)
    return (
        centered * lax.rsqrt(jnp.mean(centered * centered, axis=-1, keepdims=True) + 1e-05) * gain
    )


def gelu_exact(values):
    return jax.nn.gelu(values, approximate=False)


def project(acts, weight):
    return jnp.einsum("bsd,de->bse", acts, weight, preferred_element_type=jnp.float32)


def back_project(grads, weight):
    return jnp.einsum("bse,de->bsd", grads, weight, preferred_element_type=jnp.float32)


def weight_grad(acts, grads):
    return jnp.einsum("bsd,bse->de", acts, grads, preferred_element_type=jnp.float32)


def across(left, right):
    return lax.dot_general(left, right, (((1,), (1,)), ((), ())), preferred_element_type=jnp.float32)


def along(left, right):
    return lax.dot_general(left, right, (((0,), (0,)), ((), ())), preferred_element_type=jnp.float32)


def plain(left, right):
    return lax.dot_general(left, right, (((1,), (0,)), ((), ())), preferred_element_type=jnp.float32)


def seen_keys(keep, keys, queries, causal):
    seen = jnp.broadcast_to(keep > 0, (keys, queries))
    if causal:
        key_at = lax.broadcasted_iota(jnp.int32, (keys, queries), 0)
        query_at = lax.broadcasted_iota(jnp.int32, (keys, queries), 1)
        seen = seen & (key_at <= query_at)
    return seen


def soft_keys(keys, queries, seen, scale):
    scores = jnp.where(seen, across(keys, queries) * scale, -1000000000.0)
    expo = jnp.exp(scores - jnp.max(scores, axis=0, keepdims=True))
    return expo * (1.0 / jnp.sum(expo, axis=0, keepdims=True))


def halves_of(values):
    lane = lax.broadcasted_iota(jnp.int32, values.shape, 1)
    in_first = lane < values.shape[1] // 2
    zero = jnp.zeros_like(values)
    return (jnp.where(in_first, values, zero), jnp.where(in_first, zero, values))


def join_halves(first, second):
    lane = lax.broadcasted_iota(jnp.int32, first.shape, 1)
    return jnp.where(lane < first.shape[1] // 2, first, second)


def attend_kernel(causal, width, joint, scale, *refs):
    if joint:
        q_ref, keep_ref, out_ref = refs
        k_ref, key_at, value_at = q_ref, width, 2 * width
    else:
        q_ref, k_ref, keep_ref, out_ref = refs
        key_at, value_at = 0, width
    count, length = k_ref.shape[1], q_ref.shape[1]
    seen = seen_keys(keep_ref[0], count, length, causal)
    pair = 2 * width // HEADS
    for at in range(0, width, pair):
        queries = q_ref[0, :, at : at + pair]
        values = k_ref[0, :, value_at + at : value_at + at + pair]
        mixed = [
            along(to_low(soft_keys(keys, queries, seen, scale)), values)
            for keys in halves_of(k_ref[0, :, key_at + at : key_at + at + pair])
        ]
        out_ref[0, :, at : at + pair] = to_low(join_halves(*mixed))


def attend_back_kernel(causal, width, joint, scale, *refs):
    if joint:
        q_ref, keep_ref, g_ref, dq_ref = refs
        k_ref, dk_ref, key_at, value_at = q_ref, dq_ref, width, 2 * width
    else:
        q_ref, k_ref, keep_ref, g_ref, dq_ref, dk_ref = refs
        key_at, value_at = 0, width
    count, length = k_ref.shape[1], q_ref.shape[1]
    seen = seen_keys(keep_ref[0], count, length, causal)
    pair = 2 * width // HEADS
    for at in range(0, width, pair):
        queries = q_ref[0, :, at : at + pair]
        grads = g_ref[0, :, at : at + pair]
        all_keys = k_ref[0, :, key_at + at : key_at + at + pair]
        all_values = k_ref[0, :, value_at + at : value_at + at + pair]
        parts = []
        for keys, values in zip(halves_of(all_keys), halves_of(all_values)):
            soft = soft_keys(keys, queries, seen, scale)
            grad_soft = across(values, grads)
            inner = jnp.sum(soft * grad_soft, axis=0, keepdims=True)
            grad_scores = to_low(jnp.where(seen, soft * (grad_soft - inner), 0.0))
            parts.append(
                (
                    along(grad_scores, all_keys) * scale,
                    plain(grad_scores, queries) * scale,
                    plain(to_low(soft), grads),
                )
            )
        grad_query, grad_key, grad_value = (join_halves(*both) for both in zip(*parts))
        dq_ref[0, :, at : at + pair] = to_low(grad_query)
        dk_ref[0, :, key_at + at : key_at + at + pair] = to_low(grad_key)
        dk_ref[0, :, value_at + at : value_at + at + pair] = to_low(grad_value)


def per_image(value):
    return pl.BlockSpec((1,) + value.shape[1:], lambda image: (image, 0, 0))


def attend(queries, memory, keep, causal):
    joint = memory is None
    width = queries.shape[2] // 3 if joint else queries.shape[2]
    operands = [queries] if joint else [queries, memory]
    operands.append(keep[:, :, None])
    out = jax.ShapeDtypeStruct(queries.shape[:2] + (width,), jnp.bfloat16)
    scale = (width // HEADS) ** (-0.5)
    return pl.pallas_call(
        functools.partial(attend_kernel, causal, width, joint, scale),
        grid=(queries.shape[0],),
        out_shape=out,
        in_specs=[per_image(value) for value in operands],
        out_specs=per_image(out),
    )(*operands)


def attend_back(grad_mixed, queries, memory, keep, causal):
    joint = memory is None
    width = grad_mixed.shape[2]
    operands = [queries] if joint else [queries, memory]
    outs = [jax.ShapeDtypeStruct(value.shape, jnp.bfloat16) for value in operands]
    operands += [keep[:, :, None], grad_mixed]
    scale = (width // HEADS) ** (-0.5)
    return pl.pallas_call(
        functools.partial(attend_back_kernel, causal, width, joint, scale),
        grid=(queries.shape[0],),
        out_shape=outs,
        in_specs=[per_image(value) for value in operands],
        out_specs=[per_image(value) for value in outs],
    )(*operands)


def attention_forward(states, gain, w_in, w_out, keep, causal):
    first = to_low(layer_norm(states, gain))
    united = to_low(project(first, w_in))
    joined = attend(united, None, keep, causal)
    hidden = states + project(joined, w_out)
    return (first, united, joined, hidden)


def feedforward_forward(states, gain, w_up, w_down):
    second = to_low(layer_norm(states, gain))
    widened = project(second, w_up)
    active = to_low(gelu_exact(widened))
    after = states + project(active, w_down)
    return (second, widened, active, after)


def attention_back(grad_after, states, gain, first, united, joined, keep, causal, w_in, w_out):
    branch = to_low(grad_after)
    g_out = weight_grad(joined, branch)
    grad_joined = to_low(back_project(branch, w_out))
    (grad_united,) = attend_back(grad_joined, united, None, keep, causal)
    g_in = weight_grad(first, grad_united)
    _, pull = jax.vjp(layer_norm, states, gain)
    grad_norm, g_gain = pull(back_project(grad_united, w_in))
    return (grad_after + grad_norm, g_in, g_out, g_gain)


def feedforward_back(grad_after, states, gain, second, widened, active, w_up, w_down):
    branch = to_low(grad_after)
    g_down = weight_grad(active, branch)
    _, pull = jax.vjp(gelu_exact, widened)
    grad_wide = to_low(pull(back_project(branch, w_down))[0])
    g_up = weight_grad(second, grad_wide)
    _, pull = jax.vjp(layer_norm, states, gain)
    grad_norm, g_gain = pull(back_project(grad_wide, w_up))
    return (grad_after + grad_norm, g_up, g_down, g_gain)


def encoder_pass(states, keep, weights):
    w_in, w_out, w_pair, w_up, w_down, gains = weights
    gains = gains.astype(jnp.float32)
    first, united, joined, hidden = attention_forward(
        states, gains[0], w_in, w_out, keep, False
    )
    second, widened, active, after = feedforward_forward(hidden, gains[1], w_up, w_down)
    final = to_low(layer_norm(after, gains[2]))
    memory = to_low(project(final, w_pair))
    return (memory, (first, united, joined, hidden, second, widened, active, after, final))


def encoder_backward(states, keep, saved, weights, grad_memory):
    w_in, w_out, w_pair, w_up, w_down, gains = weights
    gains = gains.astype(jnp.float32)
    first, united, joined, hidden, second, widened, active, after, final = saved
    g_pair = weight_grad(final, grad_memory)
    _, pull = jax.vjp(layer_norm, after, gains[2])
    grad_after, g_final = pull(back_project(grad_memory, w_pair))
    grad_hidden, g_up, g_down, g_second = feedforward_back(
        grad_after, hidden, gains[1], second, widened, active, w_up, w_down
    )
    grad_states, g_in, g_out, g_first = attention_back(
        grad_hidden, states, gains[0], first, united, joined, keep, False, w_in, w_out
    )
    return (
        grad_states,
        (g_in, g_out, g_pair, g_up, g_down, jnp.stack([g_first, g_second, g_final])),
    )


def decoder_step(text, text_keep, memory, keep, weights, cotan):
    w_in, w_out, w_pair, w_up, w_down, gains = weights
    gains = gains.astype(jnp.float32)
    width = text.shape[2]
    first, united, joined, hidden = attention_forward(
        text, gains[0], w_in, w_out, text_keep, True
    )
    second = to_low(layer_norm(hidden, gains[1]))
    cross_query = to_low(project(second, w_pair[:, :width]))
    cross_joined = attend(cross_query, memory, keep, False)
    crossed = hidden + project(cross_joined, w_pair[:, width:])
    third, widened, active, output = feedforward_forward(crossed, gains[2], w_up, w_down)
    grad_crossed, g_up, g_down, g_third = feedforward_back(
        cotan, crossed, gains[2], third, widened, active, w_up, w_down
    )
    branch = to_low(grad_crossed)
    g_cross_out = weight_grad(cross_joined, branch)
    grad_cross_joined = to_low(back_project(branch, w_pair[:, width:]))
    grad_cross_query, grad_memory = attend_back(
        grad_cross_joined, cross_query, memory, keep, False
    )
    g_cross_query = weight_grad(second, grad_cross_query)
    _, pull = jax.vjp(layer_norm, hidden, gains[1])
    grad_norm, g_second = pull(back_project(grad_cross_query, w_pair[:, :width]))
    grad_hidden = grad_crossed + grad_norm
    grad_text, g_in, g_out, g_first = attention_back(
        grad_hidden, text, gains[0], first, united, joined, text_keep, True, w_in, w_out
    )
    g_pair = jnp.concatenate([g_cross_query, g_cross_out], axis=1)
    return (
        output,
        grad_text,
        grad_memory,
        (g_in, g_out, g_pair, g_up, g_down, jnp.stack([g_first, g_second, g_third])),
    )


def to_whole_images(values, section):
    half = values.shape[0] // 2
    low_part, high_part = values[:half], values[half:]
    incoming = partner(jnp.where(section == 0, high_part, low_part), "section", 0)
    kept = jnp.where(section == 0, low_part, high_part)
    left = jnp.where(section == 0, kept, incoming)
    right = jnp.where(section == 0, incoming, kept)
    return jnp.concatenate([left, right], axis=-1)


def to_half_features(values, section):
    half = values.shape[-1] // 2
    left, right = values[..., :half], values[..., half:]
    incoming = partner(jnp.where(section == 0, right, left), "section", 0)
    kept = jnp.where(section == 0, left, right)
    low_part = jnp.where(section == 0, kept, incoming)
    high_part = jnp.where(section == 0, incoming, kept)
    return jnp.concatenate([low_part, high_part], axis=0)


def ring_place(shard, size):
    column = shard % 2
    row = shard // 2
    return row * (1 - column) + (size - 1 - row) * column


def ring_shard(place, size):
    column = place // (size // 2)
    row = place * (1 - column) + (size - 1 - place) * column
    return 2 * row + column


def reduce_kernel(size, reps, kinds, *refs):
    firsts, seconds, outs, owned, paired, slots, sides = (
        refs[at * kinds : (at + 1) * kinds] for at in range(7)
    )
    send, recv, side_send, side_recv, keep, pair_send, pair_recv = refs[7 * kinds :]
    place = ring_place(lax.axis_index("dp"), size)
    replica, section = lax.axis_index("rep"), lax.axis_index("section")
    targets = (
        ring_shard((place + 1) % size, size),
        ring_shard((place + size - 1) % size, size),
    )
    signs = (-1, 1)

    barrier = pltpu.get_barrier_semaphore()
    for target in targets:
        pl.semaphore_signal(barrier, inc=1, device_id={"dp": target}, device_id_type=MESH_IDS)
    for other in range(1, reps):
        pl.semaphore_signal(
            barrier,
            inc=1,
            device_id={"rep": (replica + other) % reps},
            device_id_type=MESH_IDS,
        )
    pl.semaphore_signal(
        barrier, inc=1, device_id={"section": 1 - section}, device_id_type=MESH_IDS
    )
    pl.semaphore_wait(barrier, 2 + reps)

    def chunk_of(way, step):
        return ring_shard((place + signs[way] * (step + 1) + 2 * size) % size, size)

    def load(source, kind, way, step):
        at = chunk_of(way, step)
        return pltpu.make_async_copy(
            source[kind].at[at, way], owned[kind].at[at, way], keep.at[kind, way, step]
        )

    def pair(source, kind, way, step):
        at = chunk_of(way, step)
        return pltpu.make_async_remote_copy(
            src_ref=source[kind].at[at, way],
            dst_ref=paired[kind].at[at, way],
            send_sem=pair_send.at[kind],
            recv_sem=pair_recv.at[kind, way, step],
            device_id={"section": 1 - section},
            device_id_type=MESH_IDS,
        )

    def spread(mine, theirs):
        def issue(step, carry):
            for kind in range(kinds):
                for way in range(2):
                    pair(theirs, kind, way, step).start()
                    load(mine, kind, way, step).start()
            return carry

        lax.fori_loop(0, size, issue, 0)

    @pl.when(section == 0)
    def _():
        spread(firsts, seconds)

    @pl.when(section == 1)
    def _():
        spread(seconds, firsts)

    def own(kind, way, step):
        load(owned, kind, way, step).wait()
        pair(owned, kind, way, step).wait_recv()
        at = chunk_of(way, step)
        mine, other = owned[kind].at[at, way], paired[kind].at[at, way]
        return mine, mine[...].astype(jnp.float32) + other[...].astype(jnp.float32)

    def hop(kind, way, step, source):
        return pltpu.make_async_remote_copy(
            src_ref=source,
            dst_ref=slots[kind].at[step, way],
            send_sem=send.at[kind, way, step],
            recv_sem=recv.at[kind, way, step],
            device_id={"dp": targets[way]},
            device_id_type=MESH_IDS,
        )

    def side(kind, other):
        return pltpu.make_async_remote_copy(
            src_ref=slots[kind].at[size - 2],
            dst_ref=sides[kind].at[other - 1],
            send_sem=side_send.at[kind, other - 1],
            recv_sem=side_recv.at[kind, other - 1],
            device_id={"rep": (replica + other) % reps},
            device_id_type=MESH_IDS,
        )

    def add(kind, way, step):
        slot = slots[kind].at[step, way]
        _, mine = own(kind, way, step + 1)
        slot[...] = (slot[...].astype(jnp.float32) + mine).astype(jnp.bfloat16)

    for kind in range(kinds):
        for way in range(2):
            source, total = own(kind, way, 0)
            source[...] = total.astype(jnp.bfloat16)
            hop(kind, way, 0, source).start()

    def walk(step, carry):
        for kind in range(kinds):
            for way in range(2):
                hop(kind, way, step, slots[kind].at[step, way]).wait_recv()
                add(kind, way, step)
                hop(kind, way, step + 1, slots[kind].at[step, way]).start()
        return carry

    lax.fori_loop(0, size - 2, walk, 0)
    for kind in range(kinds):
        for way in range(2):
            hop(kind, way, size - 2, slots[kind].at[size - 2, way]).wait_recv()
            add(kind, way, size - 2)
        for other in range(1, reps):
            side(kind, other).start()
    for kind in range(kinds):
        total = slots[kind][size - 2].astype(jnp.float32)
        for other in range(1, reps):
            side(kind, other).wait_recv()
            total += sides[kind][other - 1].astype(jnp.float32)
        outs[kind][...] = total

    def drain(step, carry):
        for kind in range(kinds):
            for way in range(2):
                hop(kind, way, step, slots[kind].at[step, way]).wait_send()
        return carry

    lax.fori_loop(0, size - 1, drain, 0)
    for kind in range(kinds):
        for other in range(1, reps):
            side(kind, other).wait_send()
        pltpu.make_async_copy(owned[kind], owned[kind], pair_send.at[kind]).wait()


def reduce_all(firsts, seconds):
    size, reps = lax.axis_size("dp"), lax.axis_size("rep")
    kinds = len(firsts)
    pieces = [g.shape[1:] for g in firsts]
    scratch = [pltpu.VMEM(g.shape, jnp.bfloat16) for g in firsts] * 2
    scratch += [pltpu.VMEM((size - 1,) + p, jnp.bfloat16) for p in pieces]
    scratch += [pltpu.VMEM((max(reps - 1, 1),) + p, jnp.bfloat16) for p in pieces]
    scratch += [pltpu.SemaphoreType.DMA((kinds, 2, size - 1))] * 2
    scratch += [pltpu.SemaphoreType.DMA((kinds, max(reps - 1, 1)))] * 2
    scratch += [pltpu.SemaphoreType.DMA((kinds, 2, size)), pltpu.SemaphoreType.DMA((kinds,))]
    scratch += [pltpu.SemaphoreType.DMA((kinds, 2, size))]
    return pl.pallas_call(
        functools.partial(reduce_kernel, size, reps, kinds),
        out_shape=[jax.ShapeDtypeStruct(p, jnp.float32) for p in pieces],
        in_specs=[pl.BlockSpec(memory_space=pl.ANY)] * (2 * kinds),
        out_specs=[pl.BlockSpec(memory_space=pltpu.VMEM)] * kinds,
        scratch_shapes=scratch,
        compiler_params=pltpu.CompilerParams(
            collective_id=0, has_side_effects=True, vmem_limit_bytes=63 * 1024 * 1024
        ),
    )(*firsts, *seconds)


def by_shard(total, dimension):
    size = lax.axis_size("dp")
    if dimension == 0:
        return total.reshape(size, 2, total.shape[0] // (2 * size), total.shape[1])
    rows, width = total.shape
    part = total.reshape(rows, size, width // size).transpose(1, 0, 2)[:, None]
    return jnp.pad(part, ((0, 0), (0, 1), (0, 16 - rows), (0, 128 - width // size)))


def gather_kernel(size, reps, kinds, cuts, *refs):
    pieces, firsts, seconds = refs[:kinds], refs[kinds : 2 * kinds], refs[2 * kinds : 3 * kinds]
    send, recv, side_send, side_recv, pair_send, pair_recv, keep = refs[3 * kinds :]
    me = lax.axis_index("dp")
    place = ring_place(me, size)
    replica, section = lax.axis_index("rep"), lax.axis_index("section")
    targets = (
        ring_shard((place + 1) % size, size),
        ring_shard((place + size - 1) % size, size),
    )
    signs = (-1, 1)
    helped = [kind for kind in range(kinds) if cuts[kind] > 1]

    barrier = pltpu.get_barrier_semaphore()
    for target in targets:
        pl.semaphore_signal(barrier, inc=1, device_id={"dp": target}, device_id_type=MESH_IDS)
    pl.semaphore_signal(
        barrier, inc=1, device_id={"section": 1 - section}, device_id_type=MESH_IDS
    )
    if helped:
        pl.semaphore_signal(
            barrier, inc=1, device_id={"rep": 1 - replica}, device_id_type=MESH_IDS
        )
    pl.semaphore_wait(barrier, 4 if helped else 3)

    def carry(mine, theirs):
        def holder(way, step):
            return ring_shard((place + signs[way] * step + size) % size, size)

        def ring_rows(kind):
            return pl.ds(replica, 2) if cuts[kind] > 1 else pl.ds(0, 1)

        def hop(kind, way, step, first=False):
            at = holder(way, step)
            source = pieces[kind] if first else mine[kind].at[at]
            return pltpu.make_async_remote_copy(
                src_ref=source.at[way, ring_rows(kind)],
                dst_ref=mine[kind].at[at, way, ring_rows(kind)],
                send_sem=send.at[kind, way, step],
                recv_sem=recv.at[kind, way, step],
                device_id={"dp": targets[way]},
                device_id_type=MESH_IDS,
            )

        def arrived(kind, way, step):
            at = holder(way, step + 1)
            return pltpu.make_async_remote_copy(
                src_ref=mine[kind].at[at, way, ring_rows(kind)],
                dst_ref=mine[kind].at[at, way, ring_rows(kind)],
                send_sem=send.at[kind, way, step],
                recv_sem=recv.at[kind, way, step],
                device_id={"dp": targets[way]},
                device_id_type=MESH_IDS,
            )

        def side(kind, way, step, part):
            region = mine[kind].at[holder(way, step), way, pl.ds(part, 1)]
            return pltpu.make_async_remote_copy(
                src_ref=region,
                dst_ref=region,
                send_sem=side_send.at[kind],
                recv_sem=side_recv.at[kind, way, step - 1],
                device_id={"rep": 1 - replica},
                device_id_type=MESH_IDS,
            )

        def pair(kind, source, target):
            return pltpu.make_async_remote_copy(
                src_ref=source,
                dst_ref=target,
                send_sem=pair_send.at[kind],
                recv_sem=pair_recv.at[kind],
                device_id={"section": 1 - section},
                device_id_type=MESH_IDS,
            )

        def forward(kind, way, step, rows):
            region = mine[kind].at[holder(way, step), way, rows]
            pair(kind, region, region).start()

        def take_side(kind, way, step):
            part = 2 * (1 - replica)
            side(kind, way, step, part).wait_recv()

        for kind in range(kinds):
            for way in range(2):
                hop(kind, way, 0, first=True).start()
        for kind in range(kinds):
            pair(kind, pieces[kind], mine[kind].at[me]).start()
            pltpu.make_async_copy(pieces[kind], mine[kind].at[me], keep.at[kind]).start()

        def settle(step, last=False, sides=True):
            for kind in range(kinds):
                for way in range(2):
                    arrived(kind, way, step).wait_recv()
                    if not last:
                        hop(kind, way, step + 1).start()
                    if cuts[kind] > 1:
                        side(kind, way, step + 1, 2 * replica).start()
                    forward(kind, way, step + 1, ring_rows(kind))
            for kind in helped if sides else []:
                for way in range(2):
                    take_side(kind, way, step)

        def settle_sides(step):
            for kind in helped:
                for way in range(2):
                    forward(kind, way, step, pl.ds(2 * (1 - replica), 1))

        settle(0, sides=False)

        def walk(step, nothing):
            settle(step)
            settle_sides(step)
            return nothing

        lax.fori_loop(1, size - 2, walk, 0)
        settle(size - 2, last=True)
        settle_sides(size - 2)
        for kind in helped:
            for way in range(2):
                take_side(kind, way, size - 1)
        settle_sides(size - 1)

        for kind in range(kinds):
            pltpu.make_async_copy(pieces[kind], mine[kind].at[me], keep.at[kind]).wait()

        def drain(step, nothing):
            for kind in range(kinds):
                for way in range(2):
                    arrived(kind, way, step).wait_send()
            return nothing

        lax.fori_loop(0, size - 1, drain, 0)
        for kind in range(kinds):
            if cuts[kind] > 1:
                sent = mine[kind].at[pl.ds(0, size - 1), :, pl.ds(2 * replica, 1)]
                pltpu.make_async_copy(sent, sent, side_send.at[kind]).wait()
            pltpu.make_async_copy(mine[kind], mine[kind], pair_send.at[kind]).wait()
            pltpu.make_async_copy(theirs[kind], theirs[kind], pair_recv.at[kind]).wait()

    @pl.when(section == 0)
    def _():
        carry(firsts, seconds)

    @pl.when(section == 1)
    def _():
        carry(seconds, firsts)


def cut_of(rows, reps):
    return 3 if reps == 2 and rows % 48 == 0 else 1


def gather_all(pieces):
    size, reps = lax.axis_size("dp"), lax.axis_size("rep")
    kinds = len(pieces)
    cuts = [cut_of(piece.shape[0], reps) for piece in pieces]
    shaped = [
        piece.reshape(2, cut, piece.shape[0] // (2 * cut), piece.shape[1])
        for piece, cut in zip(pieces, cuts)
    ]
    wholes = [jax.ShapeDtypeStruct((size,) + piece.shape, piece.dtype) for piece in shaped]
    scratch = [pltpu.SemaphoreType.DMA((kinds, 2, size - 1))] * 2
    scratch += [pltpu.SemaphoreType.DMA((kinds,)), pltpu.SemaphoreType.DMA((kinds, 2, size - 1))]
    scratch += [pltpu.SemaphoreType.DMA((kinds,))] * 3
    outs = pl.pallas_call(
        functools.partial(gather_kernel, size, reps, kinds, cuts),
        out_shape=wholes * 2,
        in_specs=[pl.BlockSpec(memory_space=pltpu.VMEM)] * kinds,
        out_specs=[pl.BlockSpec(memory_space=pl.ANY)] * (2 * kinds),
        scratch_shapes=scratch,
        compiler_params=pltpu.CompilerParams(collective_id=1, has_side_effects=True),
    )(*shaped)
    return outs[:kinds], outs[kinds:]


def as_weights(outs, rows, width):
    weights = [part.reshape(-1, part.shape[-1]) for part in outs[:-1]]
    gains = outs[-1].reshape(outs[-1].shape[0], -1, outs[-1].shape[-1])[:, :rows, :width]
    return tuple(weights) + (gains.transpose(1, 0, 2).reshape(rows, -1),)


def local(
    patches,
    captions,
    tissue_keep,
    caption_mask,
    mixing,
    merging,
    crossing,
    widening,
    narrowing,
    scales,
    cotangent,
):
    section = lax.axis_index("section")
    count = patches.shape[1]
    length = captions.shape[1]
    rows, width = scales.shape[1:]
    gains = jnp.pad(scales[0], ((0, 48 - rows), (0, 128 - width)))
    firsts, seconds = gather_all(
        [mixing[0], merging[0], crossing[0], widening[0], narrowing[0], gains]
    )
    enc_weights = as_weights(firsts, rows, width)
    dec_weights = as_weights(seconds, rows, width)
    states = to_whole_images(jnp.concatenate([patches, captions, cotangent], axis=1), section)
    states = states.astype(jnp.float32)
    own_patches = states[:, :count]
    own_text = states[:, count : count + length]
    own_cotan = states[:, count + length :]
    own = own_patches.shape[0]
    keep = lax.dynamic_slice_in_dim(tissue_keep, section * own, own, 0)
    text_keep = lax.dynamic_slice_in_dim(caption_mask, section * own, own, 0)
    memory, saved = encoder_pass(own_patches, keep, enc_weights)
    output, grad_text, grad_memory, dec_grads = decoder_step(
        own_text, text_keep, memory, keep, dec_weights, own_cotan
    )
    grad_patches, enc_grads = encoder_backward(
        own_patches, keep, saved, enc_weights, grad_memory
    )
    results = to_half_features(
        jnp.concatenate([to_low(grad_patches), to_low(output), to_low(grad_text)], axis=1),
        section,
    )
    reduced = reduce_all(
        *(
            [by_shard(to_low(g), dimension) for g, dimension in zip(grads, (0, 0, 0, 0, 0, 1))]
            for grads in (enc_grads, dec_grads)
        )
    )
    summed = tuple(part.reshape(1, -1, part.shape[-1]) for part in reduced[:-1])
    summed += (reduced[-1][:1, :rows, :width],)
    return (
        results[:, count : count + length],
        results[:, count + length :],
        results[:, :count],
    ) + summed


def solution(mesh):
    in_specs = (
        P(("dp", "rep"), None, "section"),
        P(("dp", "rep"), None, "section"),
        P(("dp", "rep"), None),
        P(("dp", "rep"), None),
        P("section", "dp", None),
        P("section", "dp", None),
        P("section", "dp", None),
        P("section", "dp", None),
        P("section", "dp", None),
        P("section", None, "dp"),
        P(("dp", "rep"), None, "section"),
    )
    out_specs = (
        P(("dp", "rep"), None, "section"),
        P(("dp", "rep"), None, "section"),
        P(("dp", "rep"), None, "section"),
        P("section", "dp", None),
        P("section", "dp", None),
        P("section", "dp", None),
        P("section", "dp", None),
        P("section", "dp", None),
        P("section", None, "dp"),
    )
    return jax.shard_map(local, mesh=mesh, in_specs=in_specs, out_specs=out_specs, check_vma=False)
```

```python
import functools

import jax
import jax.numpy as jnp
from jax import lax
from jax.experimental import pallas as pl
from jax.experimental.pallas import tpu as pltpu
from jax.sharding import PartitionSpec as P

HEADS = 12
MESH_IDS = pl.DeviceIdType.MESH


def partner(value, axis, distance):
    mask = 2**distance
    pairs = [(source, source ^ mask) for source in range(lax.axis_size(axis))]
    return lax.ppermute(value, axis, pairs)


def to_low(values):
    return values.astype(jnp.bfloat16)


def layer_norm(values, gain):
    centered = values - jnp.mean(values, axis=-1, keepdims=True)
    return (
        centered * lax.rsqrt(jnp.mean(centered * centered, axis=-1, keepdims=True) + 1e-05) * gain
    )


def gelu_exact(values):
    return jax.nn.gelu(values, approximate=False)


def project(acts, weight):
    return jnp.einsum("bsd,de->bse", acts, weight, preferred_element_type=jnp.float32)


def back_project(grads, weight):
    return jnp.einsum("bse,de->bsd", grads, weight, preferred_element_type=jnp.float32)


def weight_grad(acts, grads):
    return jnp.einsum("bsd,bse->de", acts, grads, preferred_element_type=jnp.float32)


def across(left, right):
    return lax.dot_general(left, right, (((1,), (1,)), ((), ())), preferred_element_type=jnp.float32)


def along(left, right):
    return lax.dot_general(left, right, (((0,), (0,)), ((), ())), preferred_element_type=jnp.float32)


def plain(left, right):
    return lax.dot_general(left, right, (((1,), (0,)), ((), ())), preferred_element_type=jnp.float32)


def seen_keys(keep, keys, queries, causal):
    seen = jnp.broadcast_to(keep > 0, (keys, queries))
    if causal:
        key_at = lax.broadcasted_iota(jnp.int32, (keys, queries), 0)
        query_at = lax.broadcasted_iota(jnp.int32, (keys, queries), 1)
        seen = seen & (key_at <= query_at)
    return seen


def soft_keys(keys, queries, seen, scale):
    scores = jnp.where(seen, across(keys, queries) * scale, -1000000000.0)
    expo = jnp.exp(scores - jnp.max(scores, axis=0, keepdims=True))
    return expo * (1.0 / jnp.sum(expo, axis=0, keepdims=True))


def halves_of(values):
    lane = lax.broadcasted_iota(jnp.int32, values.shape, 1)
    in_first = lane < values.shape[1] // 2
    zero = jnp.zeros_like(values)
    return (jnp.where(in_first, values, zero), jnp.where(in_first, zero, values))


def join_halves(first, second):
    lane = lax.broadcasted_iota(jnp.int32, first.shape, 1)
    return jnp.where(lane < first.shape[1] // 2, first, second)


def attend_kernel(causal, width, joint, scale, *refs):
    if joint:
        q_ref, keep_ref, out_ref = refs
        k_ref, key_at, value_at = q_ref, width, 2 * width
    else:
        q_ref, k_ref, keep_ref, out_ref = refs
        key_at, value_at = 0, width
    count, length = k_ref.shape[1], q_ref.shape[1]
    seen = seen_keys(keep_ref[0], count, length, causal)
    pair = 2 * width // HEADS
    for at in range(0, width, pair):
        queries = q_ref[0, :, at : at + pair]
        values = k_ref[0, :, value_at + at : value_at + at + pair]
        mixed = [
            along(to_low(soft_keys(keys, queries, seen, scale)), values)
            for keys in halves_of(k_ref[0, :, key_at + at : key_at + at + pair])
        ]
        out_ref[0, :, at : at + pair] = to_low(join_halves(*mixed))


def attend_back_kernel(causal, width, joint, scale, *refs):
    if joint:
        q_ref, keep_ref, g_ref, dq_ref = refs
        k_ref, dk_ref, key_at, value_at = q_ref, dq_ref, width, 2 * width
    else:
        q_ref, k_ref, keep_ref, g_ref, dq_ref, dk_ref = refs
        key_at, value_at = 0, width
    count, length = k_ref.shape[1], q_ref.shape[1]
    seen = seen_keys(keep_ref[0], count, length, causal)
    pair = 2 * width // HEADS
    for at in range(0, width, pair):
        queries = q_ref[0, :, at : at + pair]
        grads = g_ref[0, :, at : at + pair]
        all_keys = k_ref[0, :, key_at + at : key_at + at + pair]
        all_values = k_ref[0, :, value_at + at : value_at + at + pair]
        parts = []
        for keys, values in zip(halves_of(all_keys), halves_of(all_values)):
            soft = soft_keys(keys, queries, seen, scale)
            grad_soft = across(values, grads)
            inner = jnp.sum(soft * grad_soft, axis=0, keepdims=True)
            grad_scores = to_low(jnp.where(seen, soft * (grad_soft - inner), 0.0))
            parts.append(
                (
                    along(grad_scores, all_keys) * scale,
                    plain(grad_scores, queries) * scale,
                    plain(to_low(soft), grads),
                )
            )
        grad_query, grad_key, grad_value = (join_halves(*both) for both in zip(*parts))
        dq_ref[0, :, at : at + pair] = to_low(grad_query)
        dk_ref[0, :, key_at + at : key_at + at + pair] = to_low(grad_key)
        dk_ref[0, :, value_at + at : value_at + at + pair] = to_low(grad_value)


def per_image(value):
    return pl.BlockSpec((1,) + value.shape[1:], lambda image: (image, 0, 0))


def attend(queries, memory, keep, causal):
    joint = memory is None
    width = queries.shape[2] // 3 if joint else queries.shape[2]
    operands = [queries] if joint else [queries, memory]
    operands.append(keep[:, :, None])
    out = jax.ShapeDtypeStruct(queries.shape[:2] + (width,), jnp.bfloat16)
    scale = (width // HEADS) ** (-0.5)
    return pl.pallas_call(
        functools.partial(attend_kernel, causal, width, joint, scale),
        grid=(queries.shape[0],),
        out_shape=out,
        in_specs=[per_image(value) for value in operands],
        out_specs=per_image(out),
    )(*operands)


def attend_back(grad_mixed, queries, memory, keep, causal):
    joint = memory is None
    width = grad_mixed.shape[2]
    operands = [queries] if joint else [queries, memory]
    outs = [jax.ShapeDtypeStruct(value.shape, jnp.bfloat16) for value in operands]
    operands += [keep[:, :, None], grad_mixed]
    scale = (width // HEADS) ** (-0.5)
    return pl.pallas_call(
        functools.partial(attend_back_kernel, causal, width, joint, scale),
        grid=(queries.shape[0],),
        out_shape=outs,
        in_specs=[per_image(value) for value in operands],
        out_specs=[per_image(value) for value in outs],
    )(*operands)


def attention_forward(states, gain, w_in, w_out, keep, causal):
    first = to_low(layer_norm(states, gain))
    united = to_low(project(first, w_in))
    joined = attend(united, None, keep, causal)
    hidden = states + project(joined, w_out)
    return (first, united, joined, hidden)


def feedforward_forward(states, gain, w_up, w_down):
    second = to_low(layer_norm(states, gain))
    widened = project(second, w_up)
    active = to_low(gelu_exact(widened))
    after = states + project(active, w_down)
    return (second, widened, active, after)


def attention_back(grad_after, states, gain, first, united, joined, keep, causal, w_in, w_out):
    branch = to_low(grad_after)
    g_out = weight_grad(joined, branch)
    grad_joined = to_low(back_project(branch, w_out))
    (grad_united,) = attend_back(grad_joined, united, None, keep, causal)
    g_in = weight_grad(first, grad_united)
    _, pull = jax.vjp(layer_norm, states, gain)
    grad_norm, g_gain = pull(back_project(grad_united, w_in))
    return (grad_after + grad_norm, g_in, g_out, g_gain)


def feedforward_back(grad_after, states, gain, second, widened, active, w_up, w_down):
    branch = to_low(grad_after)
    g_down = weight_grad(active, branch)
    _, pull = jax.vjp(gelu_exact, widened)
    grad_wide = to_low(pull(back_project(branch, w_down))[0])
    g_up = weight_grad(second, grad_wide)
    _, pull = jax.vjp(layer_norm, states, gain)
    grad_norm, g_gain = pull(back_project(grad_wide, w_up))
    return (grad_after + grad_norm, g_up, g_down, g_gain)


def encoder_pass(states, keep, weights):
    w_in, w_out, w_pair, w_up, w_down, gains = weights
    gains = gains.astype(jnp.float32)
    first, united, joined, hidden = attention_forward(
        states, gains[0], w_in, w_out, keep, False
    )
    second, widened, active, after = feedforward_forward(hidden, gains[1], w_up, w_down)
    final = to_low(layer_norm(after, gains[2]))
    memory = to_low(project(final, w_pair))
    return (memory, (first, united, joined, hidden, second, widened, active, after, final))


def encoder_backward(states, keep, saved, weights, grad_memory):
    w_in, w_out, w_pair, w_up, w_down, gains = weights
    gains = gains.astype(jnp.float32)
    first, united, joined, hidden, second, widened, active, after, final = saved
    g_pair = weight_grad(final, grad_memory)
    _, pull = jax.vjp(layer_norm, after, gains[2])
    grad_after, g_final = pull(back_project(grad_memory, w_pair))
    grad_hidden, g_up, g_down, g_second = feedforward_back(
        grad_after, hidden, gains[1], second, widened, active, w_up, w_down
    )
    grad_states, g_in, g_out, g_first = attention_back(
        grad_hidden, states, gains[0], first, united, joined, keep, False, w_in, w_out
    )
    return (
        grad_states,
        (g_in, g_out, g_pair, g_up, g_down, jnp.stack([g_first, g_second, g_final])),
    )


def decoder_step(text, text_keep, memory, keep, weights, cotan):
    w_in, w_out, w_pair, w_up, w_down, gains = weights
    gains = gains.astype(jnp.float32)
    width = text.shape[2]
    first, united, joined, hidden = attention_forward(
        text, gains[0], w_in, w_out, text_keep, True
    )
    second = to_low(layer_norm(hidden, gains[1]))
    cross_query = to_low(project(second, w_pair[:, :width]))
    cross_joined = attend(cross_query, memory, keep, False)
    crossed = hidden + project(cross_joined, w_pair[:, width:])
    third, widened, active, output = feedforward_forward(crossed, gains[2], w_up, w_down)
    grad_crossed, g_up, g_down, g_third = feedforward_back(
        cotan, crossed, gains[2], third, widened, active, w_up, w_down
    )
    branch = to_low(grad_crossed)
    g_cross_out = weight_grad(cross_joined, branch)
    grad_cross_joined = to_low(back_project(branch, w_pair[:, width:]))
    grad_cross_query, grad_memory = attend_back(
        grad_cross_joined, cross_query, memory, keep, False
    )
    g_cross_query = weight_grad(second, grad_cross_query)
    _, pull = jax.vjp(layer_norm, hidden, gains[1])
    grad_norm, g_second = pull(back_project(grad_cross_query, w_pair[:, :width]))
    grad_hidden = grad_crossed + grad_norm
    grad_text, g_in, g_out, g_first = attention_back(
        grad_hidden, text, gains[0], first, united, joined, text_keep, True, w_in, w_out
    )
    g_pair = jnp.concatenate([g_cross_query, g_cross_out], axis=1)
    return (
        output,
        grad_text,
        grad_memory,
        (g_in, g_out, g_pair, g_up, g_down, jnp.stack([g_first, g_second, g_third])),
    )


def to_whole_images(values, section):
    half = values.shape[0] // 2
    low_part, high_part = values[:half], values[half:]
    incoming = partner(jnp.where(section == 0, high_part, low_part), "section", 0)
    kept = jnp.where(section == 0, low_part, high_part)
    left = jnp.where(section == 0, kept, incoming)
    right = jnp.where(section == 0, incoming, kept)
    return jnp.concatenate([left, right], axis=-1)


def to_half_features(values, section):
    half = values.shape[-1] // 2
    left, right = values[..., :half], values[..., half:]
    incoming = partner(jnp.where(section == 0, right, left), "section", 0)
    kept = jnp.where(section == 0, left, right)
    low_part = jnp.where(section == 0, kept, incoming)
    high_part = jnp.where(section == 0, incoming, kept)
    return jnp.concatenate([low_part, high_part], axis=0)


def ring_place(shard, size):
    column = shard % 2
    row = shard // 2
    return row * (1 - column) + (size - 1 - row) * column


def ring_shard(place, size):
    column = place // (size // 2)
    row = place * (1 - column) + (size - 1 - place) * column
    return 2 * row + column


def reduce_kernel(size, reps, kinds, early, *refs):
    firsts, seconds, outs, owned, paired, slots, sides = (
        refs[at * kinds : (at + 1) * kinds] for at in range(7)
    )
    crossed = dict(zip(early, refs[7 * kinds :]))
    late = [kind for kind in range(kinds) if kind not in early]
    send, recv, side_send, side_recv, keep, pair_send, pair_recv, cross_send, cross_recv = refs[
        7 * kinds + len(early) :
    ]
    place = ring_place(lax.axis_index("dp"), size)
    replica, section = lax.axis_index("rep"), lax.axis_index("section")
    targets = (
        ring_shard((place + 1) % size, size),
        ring_shard((place + size - 1) % size, size),
    )
    signs = (-1, 1)

    barrier = pltpu.get_barrier_semaphore()
    for target in targets:
        pl.semaphore_signal(barrier, inc=1, device_id={"dp": target}, device_id_type=MESH_IDS)
    for other in range(1, reps):
        pl.semaphore_signal(
            barrier,
            inc=1,
            device_id={"rep": (replica + other) % reps},
            device_id_type=MESH_IDS,
        )
    pl.semaphore_signal(
        barrier, inc=1, device_id={"section": 1 - section}, device_id_type=MESH_IDS
    )
    pl.semaphore_wait(barrier, 2 + reps)

    def chunk_of(way, step):
        return ring_shard((place + signs[way] * (step + 1) + 2 * size) % size, size)

    def load(source, kind, way, step):
        at = chunk_of(way, step)
        return pltpu.make_async_copy(
            source[kind].at[at, way], owned[kind].at[at, way], keep.at[kind, way, step]
        )

    def pair(source, kind, way, step):
        at = chunk_of(way, step)
        return pltpu.make_async_remote_copy(
            src_ref=source[kind].at[at, way],
            dst_ref=paired[kind].at[at, way],
            send_sem=pair_send.at[kind],
            recv_sem=pair_recv.at[kind, way, step],
            device_id={"section": 1 - section},
            device_id_type=MESH_IDS,
        )

    def spread(mine, theirs):
        def issue(step, carry):
            for kind in range(kinds):
                for way in range(2):
                    pair(theirs, kind, way, step).start()
                    load(mine, kind, way, step).start()
            return carry

        lax.fori_loop(0, size, issue, 0)

    @pl.when(section == 0)
    def _():
        spread(firsts, seconds)

    @pl.when(section == 1)
    def _():
        spread(seconds, firsts)

    def part_of(kind):
        return replica if kind in early else 0

    def settled(kind, way, step):
        load(owned, kind, way, step).wait()
        pair(owned, kind, way, step).wait_recv()

    def both(kind, way, step, part):
        at = chunk_of(way, step)
        mine, other = owned[kind].at[at, way, part], paired[kind].at[at, way, part]
        return mine, mine[...].astype(jnp.float32) + other[...].astype(jnp.float32)

    def cross(kind, way, step):
        at = chunk_of(way, step)
        return pltpu.make_async_remote_copy(
            src_ref=owned[kind].at[at, way, 1 - replica],
            dst_ref=crossed[kind].at[at, way],
            send_sem=cross_send.at[kind],
            recv_sem=cross_recv.at[kind, way, step],
            device_id={"rep": 1 - replica},
            device_id_type=MESH_IDS,
        )

    def give(step):
        for kind in early:
            for way in range(2):
                settled(kind, way, step)
                source, total = both(kind, way, step, 1 - replica)
                source[...] = total.astype(jnp.bfloat16)
                cross(kind, way, step).start()

    def own(kind, way, step):
        if kind not in early:
            settled(kind, way, step)
            return both(kind, way, step, 0)
        cross(kind, way, step).wait_recv()
        source, total = both(kind, way, step, replica)
        return source, total + crossed[kind][chunk_of(way, step), way].astype(jnp.float32)

    def hop(kind, way, step, source):
        return pltpu.make_async_remote_copy(
            src_ref=source,
            dst_ref=slots[kind].at[step, way],
            send_sem=send.at[kind, way, step],
            recv_sem=recv.at[kind, way, step],
            device_id={"dp": targets[way]},
            device_id_type=MESH_IDS,
        )

    def side(kind, other):
        return pltpu.make_async_remote_copy(
            src_ref=slots[kind].at[size - 2],
            dst_ref=sides[kind].at[other - 1],
            send_sem=side_send.at[kind, other - 1],
            recv_sem=side_recv.at[kind, other - 1],
            device_id={"rep": (replica + other) % reps},
            device_id_type=MESH_IDS,
        )

    def add(kind, way, step):
        slot = slots[kind].at[step, way]
        _, mine = own(kind, way, step + 1)
        slot[...] = (slot[...].astype(jnp.float32) + mine).astype(jnp.bfloat16)

    def begin(group):
        for kind in group:
            for way in range(2):
                source, total = own(kind, way, 0)
                source[...] = total.astype(jnp.bfloat16)
                hop(kind, way, 0, source).start()

    def advance(group, step, last):
        for kind in group:
            for way in range(2):
                hop(kind, way, step, slots[kind].at[step, way]).wait_recv()
                add(kind, way, step)
                if not last:
                    hop(kind, way, step + 1, slots[kind].at[step, way]).start()

    def finish(group):
        advance(group, size - 2, True)
        for kind in group:
            for other in range(1, reps):
                side(kind, other).start()

    begin(late)

    def walk_late(step, carry):
        if early:

            @pl.when(step < size // 2)
            def _():
                give(2 * step)
                give(2 * step + 1)

        advance(late, step, False)
        return carry

    lax.fori_loop(0, size - 2, walk_late, 0)
    finish(late)
    if early:
        begin(early)

        def walk_early(step, carry):
            advance(early, step, False)
            return carry

        lax.fori_loop(0, size - 2, walk_early, 0)
        finish(early)
    for kind in late:
        total = slots[kind][size - 2].astype(jnp.float32)
        for other in range(1, reps):
            side(kind, other).wait_recv()
            total += sides[kind][other - 1].astype(jnp.float32)
        outs[kind][:, 0] = total
    for kind in early:
        side(kind, 1).wait_recv()
        for way in range(2):
            mine, theirs = outs[kind].at[way, replica], outs[kind].at[way, 1 - replica]
            mine[...] = slots[kind][size - 2, way].astype(jnp.float32)
            theirs[...] = sides[kind][0, way].astype(jnp.float32)

    def drain(step, carry):
        for kind in range(kinds):
            for way in range(2):
                hop(kind, way, step, slots[kind].at[step, way]).wait_send()
        return carry

    lax.fori_loop(0, size - 1, drain, 0)
    for kind in range(kinds):
        for other in range(1, reps):
            side(kind, other).wait_send()
        pltpu.make_async_copy(owned[kind], owned[kind], pair_send.at[kind]).wait()
    for kind in early:
        pltpu.make_async_copy(crossed[kind], crossed[kind], cross_send.at[kind]).wait()


def reduce_all(firsts, seconds):
    size, reps = lax.axis_size("dp"), lax.axis_size("rep")
    kinds = len(firsts)
    early = [kind for kind in range(kinds) if firsts[kind].shape[2] > 1]
    pieces = [(2,) + g.shape[3:] for g in firsts]
    scratch = [pltpu.VMEM(g.shape, jnp.bfloat16) for g in firsts] * 2
    scratch += [pltpu.VMEM((size - 1,) + p, jnp.bfloat16) for p in pieces]
    scratch += [pltpu.VMEM((max(reps - 1, 1),) + p, jnp.bfloat16) for p in pieces]
    scratch += [pltpu.VMEM((size,) + pieces[kind], jnp.bfloat16) for kind in early]
    scratch += [pltpu.SemaphoreType.DMA((kinds, 2, size - 1))] * 2
    scratch += [pltpu.SemaphoreType.DMA((kinds, max(reps - 1, 1)))] * 2
    scratch += [pltpu.SemaphoreType.DMA((kinds, 2, size)), pltpu.SemaphoreType.DMA((kinds,))]
    scratch += [pltpu.SemaphoreType.DMA((kinds, 2, size))]
    scratch += [pltpu.SemaphoreType.DMA((kinds,)), pltpu.SemaphoreType.DMA((kinds, 2, size))]
    return pl.pallas_call(
        functools.partial(reduce_kernel, size, reps, kinds, early),
        out_shape=[jax.ShapeDtypeStruct(g.shape[1:], jnp.float32) for g in firsts],
        in_specs=[pl.BlockSpec(memory_space=pl.ANY)] * (2 * kinds),
        out_specs=[pl.BlockSpec(memory_space=pltpu.VMEM)] * kinds,
        scratch_shapes=scratch,
        compiler_params=pltpu.CompilerParams(
            collective_id=0, has_side_effects=True, vmem_limit_bytes=63 * 1024 * 1024
        ),
    )(*firsts, *seconds)


def by_shard(total, dimension, early):
    size, reps = lax.axis_size("dp"), lax.axis_size("rep")
    if dimension == 0:
        half = total.shape[0] // (2 * size)
        cut = 2 if early and reps == 2 and half % 16 == 0 else 1
        return total.reshape(size, 2, cut, half // cut, total.shape[1])
    rows, width = total.shape
    part = total.reshape(rows, size, width // size).transpose(1, 0, 2)[:, None, None]
    return jnp.pad(part, ((0, 0), (0, 1), (0, 0), (0, 16 - rows), (0, 128 - width // size)))


def gather_kernel(size, reps, kinds, cuts, *refs):
    pieces, firsts, seconds = refs[:kinds], refs[kinds : 2 * kinds], refs[2 * kinds : 3 * kinds]
    send, recv, side_send, side_recv, pair_send, pair_recv, keep = refs[3 * kinds :]
    me = lax.axis_index("dp")
    place = ring_place(me, size)
    replica, section = lax.axis_index("rep"), lax.axis_index("section")
    targets = (
        ring_shard((place + 1) % size, size),
        ring_shard((place + size - 1) % size, size),
    )
    signs = (-1, 1)
    helped = [kind for kind in range(kinds) if cuts[kind] > 1]

    barrier = pltpu.get_barrier_semaphore()
    for target in targets:
        pl.semaphore_signal(barrier, inc=1, device_id={"dp": target}, device_id_type=MESH_IDS)
    pl.semaphore_signal(
        barrier, inc=1, device_id={"section": 1 - section}, device_id_type=MESH_IDS
    )
    if helped:
        pl.semaphore_signal(
            barrier, inc=1, device_id={"rep": 1 - replica}, device_id_type=MESH_IDS
        )
    pl.semaphore_wait(barrier, 4 if helped else 3)

    def carry(mine, theirs):
        def holder(way, step):
            return ring_shard((place + signs[way] * step + size) % size, size)

        def ring_rows(kind):
            return pl.ds(replica, 2) if cuts[kind] > 1 else pl.ds(0, 1)

        def hop(kind, way, step, first=False):
            at = holder(way, step)
            source = pieces[kind] if first else mine[kind].at[at]
            return pltpu.make_async_remote_copy(
                src_ref=source.at[way, ring_rows(kind)],
                dst_ref=mine[kind].at[at, way, ring_rows(kind)],
                send_sem=send.at[kind, way, step],
                recv_sem=recv.at[kind, way, step],
                device_id={"dp": targets[way]},
                device_id_type=MESH_IDS,
            )

        def arrived(kind, way, step):
            at = holder(way, step + 1)
            return pltpu.make_async_remote_copy(
                src_ref=mine[kind].at[at, way, ring_rows(kind)],
                dst_ref=mine[kind].at[at, way, ring_rows(kind)],
                send_sem=send.at[kind, way, step],
                recv_sem=recv.at[kind, way, step],
                device_id={"dp": targets[way]},
                device_id_type=MESH_IDS,
            )

        def side(kind, way, step, part):
            region = mine[kind].at[holder(way, step), way, pl.ds(part, 1)]
            return pltpu.make_async_remote_copy(
                src_ref=region,
                dst_ref=region,
                send_sem=side_send.at[kind],
                recv_sem=side_recv.at[kind, way, step - 1],
                device_id={"rep": 1 - replica},
                device_id_type=MESH_IDS,
            )

        def pair(kind, source, target):
            return pltpu.make_async_remote_copy(
                src_ref=source,
                dst_ref=target,
                send_sem=pair_send.at[kind],
                recv_sem=pair_recv.at[kind],
                device_id={"section": 1 - section},
                device_id_type=MESH_IDS,
            )

        def forward(kind, way, step, rows):
            region = mine[kind].at[holder(way, step), way, rows]
            pair(kind, region, region).start()

        def take_side(kind, way, step):
            part = 2 * (1 - replica)
            side(kind, way, step, part).wait_recv()

        for kind in range(kinds):
            for way in range(2):
                hop(kind, way, 0, first=True).start()
        for kind in range(kinds):
            pair(kind, pieces[kind], mine[kind].at[me]).start()
            pltpu.make_async_copy(pieces[kind], mine[kind].at[me], keep.at[kind]).start()

        def settle(step, last=False, sides=True):
            for kind in range(kinds):
                for way in range(2):
                    arrived(kind, way, step).wait_recv()
                    if not last:
                        hop(kind, way, step + 1).start()
                    if cuts[kind] > 1:
                        side(kind, way, step + 1, 2 * replica).start()
                    forward(kind, way, step + 1, ring_rows(kind))
            for kind in helped if sides else []:
                for way in range(2):
                    take_side(kind, way, step)

        def settle_sides(step):
            for kind in helped:
                for way in range(2):
                    forward(kind, way, step, pl.ds(2 * (1 - replica), 1))

        settle(0, sides=False)

        def walk(step, nothing):
            settle(step)
            settle_sides(step)
            return nothing

        lax.fori_loop(1, size - 2, walk, 0)
        settle(size - 2, last=True)
        settle_sides(size - 2)
        for kind in helped:
            for way in range(2):
                take_side(kind, way, size - 1)
        settle_sides(size - 1)

        for kind in range(kinds):
            pltpu.make_async_copy(pieces[kind], mine[kind].at[me], keep.at[kind]).wait()

        def drain(step, nothing):
            for kind in range(kinds):
                for way in range(2):
                    arrived(kind, way, step).wait_send()
            return nothing

        lax.fori_loop(0, size - 1, drain, 0)
        for kind in range(kinds):
            if cuts[kind] > 1:
                sent = mine[kind].at[pl.ds(0, size - 1), :, pl.ds(2 * replica, 1)]
                pltpu.make_async_copy(sent, sent, side_send.at[kind]).wait()
            pltpu.make_async_copy(mine[kind], mine[kind], pair_send.at[kind]).wait()
            pltpu.make_async_copy(theirs[kind], theirs[kind], pair_recv.at[kind]).wait()

    @pl.when(section == 0)
    def _():
        carry(firsts, seconds)

    @pl.when(section == 1)
    def _():
        carry(seconds, firsts)


def cut_of(rows, reps):
    return 3 if reps == 2 and rows % 48 == 0 else 1


def gather_all(pieces):
    size, reps = lax.axis_size("dp"), lax.axis_size("rep")
    kinds = len(pieces)
    cuts = [cut_of(piece.shape[0], reps) for piece in pieces]
    shaped = [
        piece.reshape(2, cut, piece.shape[0] // (2 * cut), piece.shape[1])
        for piece, cut in zip(pieces, cuts)
    ]
    wholes = [jax.ShapeDtypeStruct((size,) + piece.shape, piece.dtype) for piece in shaped]
    scratch = [pltpu.SemaphoreType.DMA((kinds, 2, size - 1))] * 2
    scratch += [pltpu.SemaphoreType.DMA((kinds,)), pltpu.SemaphoreType.DMA((kinds, 2, size - 1))]
    scratch += [pltpu.SemaphoreType.DMA((kinds,))] * 3
    outs = pl.pallas_call(
        functools.partial(gather_kernel, size, reps, kinds, cuts),
        out_shape=wholes * 2,
        in_specs=[pl.BlockSpec(memory_space=pltpu.VMEM)] * kinds,
        out_specs=[pl.BlockSpec(memory_space=pl.ANY)] * (2 * kinds),
        scratch_shapes=scratch,
        compiler_params=pltpu.CompilerParams(collective_id=1, has_side_effects=True),
    )(*shaped)
    return outs[:kinds], outs[kinds:]


def as_weights(outs, rows, width):
    weights = [part.reshape(-1, part.shape[-1]) for part in outs[:-1]]
    gains = outs[-1].reshape(outs[-1].shape[0], -1, outs[-1].shape[-1])[:, :rows, :width]
    return tuple(weights) + (gains.transpose(1, 0, 2).reshape(rows, -1),)


def local(
    patches,
    captions,
    tissue_keep,
    caption_mask,
    mixing,
    merging,
    crossing,
    widening,
    narrowing,
    scales,
    cotangent,
):
    section = lax.axis_index("section")
    count = patches.shape[1]
    length = captions.shape[1]
    rows, width = scales.shape[1:]
    gains = jnp.pad(scales[0], ((0, 48 - rows), (0, 128 - width)))
    firsts, seconds = gather_all(
        [mixing[0], merging[0], crossing[0], widening[0], narrowing[0], gains]
    )
    enc_weights = as_weights(firsts, rows, width)
    dec_weights = as_weights(seconds, rows, width)
    states = to_whole_images(jnp.concatenate([patches, captions, cotangent], axis=1), section)
    states = states.astype(jnp.float32)
    own_patches = states[:, :count]
    own_text = states[:, count : count + length]
    own_cotan = states[:, count + length :]
    own = own_patches.shape[0]
    keep = lax.dynamic_slice_in_dim(tissue_keep, section * own, own, 0)
    text_keep = lax.dynamic_slice_in_dim(caption_mask, section * own, own, 0)
    memory, saved = encoder_pass(own_patches, keep, enc_weights)
    output, grad_text, grad_memory, dec_grads = decoder_step(
        own_text, text_keep, memory, keep, dec_weights, own_cotan
    )
    grad_patches, enc_grads = encoder_backward(
        own_patches, keep, saved, enc_weights, grad_memory
    )
    results = to_half_features(
        jnp.concatenate([to_low(grad_patches), to_low(output), to_low(grad_text)], axis=1),
        section,
    )
    reduced = reduce_all(
        *(
            [
                by_shard(to_low(g), dimension, at in (1, 2, 3))
                for at, (g, dimension) in enumerate(zip(grads, (0, 0, 0, 0, 0, 1)))
            ]
            for grads in (enc_grads, dec_grads)
        )
    )
    summed = tuple(part.reshape(1, -1, part.shape[-1]) for part in reduced[:-1])
    summed += (reduced[-1][0, :, :rows, :width],)
    return (
        results[:, count : count + length],
        results[:, count + length :],
        results[:, :count],
    ) + summed


def solution(mesh):
    in_specs = (
        P(("dp", "rep"), None, "section"),
        P(("dp", "rep"), None, "section"),
        P(("dp", "rep"), None),
        P(("dp", "rep"), None),
        P("section", "dp", None),
        P("section", "dp", None),
        P("section", "dp", None),
        P("section", "dp", None),
        P("section", "dp", None),
        P("section", None, "dp"),
        P(("dp", "rep"), None, "section"),
    )
    out_specs = (
        P(("dp", "rep"), None, "section"),
        P(("dp", "rep"), None, "section"),
        P(("dp", "rep"), None, "section"),
        P("section", "dp", None),
        P("section", "dp", None),
        P("section", "dp", None),
        P("section", "dp", None),
        P("section", "dp", None),
        P("section", None, "dp"),
    )
    return jax.shard_map(local, mesh=mesh, in_specs=in_specs, out_specs=out_specs, check_vma=False)
```
